32 devices in a mesh: batch: 2 (over x), row: 4 (over z), col: 4 (over y, core).
Axes of the slice: x: 2, y: 2, z: 4, core: 2. Of those that a mesh axis runs over, the one named last changes fastest.
Arguments:
- l_mat: bfloat16 [16384, 8192], P(('batch', 'row'), 'col'), parts along dimension 0
- b_mat: bfloat16 [16384, 16384], P(('batch', 'row'), 'col'), parts along dimension 0
Outputs:
- output: bfloat16 [16384, 16384], P(('batch', 'row'), 'col'), parts along dimension 0
There are 2 independent parts. The reference program is written for one: setup_inputs(seed, part) draws one part's arguments, and reference() takes and returns one part's arrays. A program takes and returns all parts, laid end to end along the dimension named above; each array names one.
All inputs are finite; a program needn't handle non-finite values.
Results may differ from the reference program's by a relative error of at most 0.001.
Values are sent between devices in bfloat16 or wider.
A program may use at most 1 GiB of HBM per device.

```python
import jax
import jax.numpy as jnp

N = 8192
M = 16384


def setup_inputs(seed: int = 0, part: int = 0) -> dict:
    base_key = jax.random.fold_in(jax.random.key(seed), part)
    key_l, key_b = jax.random.split(base_key)
    row_scale = 1.0 / jnp.sqrt(jnp.arange(N, dtype=jnp.float32) + 1.0)
    l_full = jax.random.normal(key_l, (N, N), jnp.float32)
    l_mat = jnp.tril(l_full) * row_scale[:, None]
    b_mat = jax.random.normal(key_b, (N, M), jnp.float32)
    return {'l_mat': l_mat.astype(jnp.bfloat16), 'b_mat': b_mat.astype(jnp.bfloat16)}


def reference(l_mat, b_mat):
    product = jnp.dot(l_mat, b_mat, preferred_element_type=jnp.float32)
    return product.astype(jnp.bfloat16)
```

```python
import functools

import jax
import jax.numpy as jnp
from jax import lax
from jax.experimental import pallas as pl
from jax.experimental.pallas import tpu as pltpu
from jax.sharding import PartitionSpec as P

MESH = pl.DeviceIdType.MESH
TILES = 4
CHUNK = 256


def mid_order(chunks):
    return [(1, c) for c in range(chunks)] + [(0, c) for c in range(chunks)]


def kernel(
    l_ref, b_ref, x_ref, rb_ref, lg_ref,
    l3_v, b_v, strip_v, x3_v, xo_v,
    b0_rx, b1_rx, b3_rx, l_rx, l3_rx, cross_rx, x3_rx,
    b_tx, fwd_tx, l_tx, l3_tx, x3_tx,
    load_sem, strip_sem, out_sem, l3_sem,
):
    n, m = b_ref.shape
    half = n // 2
    rt = n // TILES
    w = CHUNK
    chunks = m // w
    batch, row, col = (lax.axis_index(a) for a in ("batch", "row", "col"))
    core_peer = col + 1 - 2 * lax.rem(col, 2)
    y_peer = lax.rem(col + 2, 4)
    far = lax.rem(core_peer + 2, 4)

    def remote(src, dst, send, recv, r, c):
        return pltpu.make_async_remote_copy(
            src_ref=src, dst_ref=dst, send_sem=send, recv_sem=recv,
            device_id=(batch, r, c), device_id_type=MESH,
        )

    def arrived(dst, sem):
        pltpu.make_async_copy(dst, dst, sem).wait()

    def own_chunk(c):
        return b_ref.at[:, pl.ds(pl.multiple_of(c * w, w), w)]

    def x_tile(i, c):
        return x_ref.at[pl.ds(i * rt, rt), pl.ds(pl.multiple_of(c * w, w), w)]

    def l_exchange_start():
        remote(l_ref, lg_ref.at[0, col], l_tx.at[0], l_rx.at[0], row, y_peer).start()
        remote(l_ref, lg_ref.at[0, col], l_tx.at[1], l_rx.at[1], row, core_peer).start()

    def l_forward():
        blk = lg_ref.at[0, y_peer]
        arrived(blk, l_rx.at[0])
        remote(blk, blk, l_tx.at[2], l_rx.at[2], row, core_peer).start()

    def l_exchange_end():
        arrived(lg_ref.at[0, core_peer], l_rx.at[1])
        arrived(lg_ref.at[0, far], l_rx.at[2])

    def l_exchange_drain():
        for s in range(3):
            arrived(l_ref, l_tx.at[s])

    def strip_parts(r, i):
        return [(k, n if k < r else (i + 1) * rt) for k in range(r + 1)]

    def strip_start(r, i):
        for k, depth in strip_parts(r, i):
            dst = strip_v.at[i % 2, :, pl.ds(k * n, depth)]
            rows = pl.ds(i * rt, rt)

            @pl.when(col == k)
            def _(dst=dst, rows=rows, depth=depth):
                pltpu.make_async_copy(l_ref.at[rows, pl.ds(0, depth)], dst, strip_sem.at[i % 2]).start()

            @pl.when(col != k)
            def _(dst=dst, rows=rows, depth=depth, k=k):
                pltpu.make_async_copy(lg_ref.at[0, k, rows, pl.ds(0, depth)], dst, strip_sem.at[i % 2]).start()

    def strip_wait(r, i):
        depth = r * n + (i + 1) * rt
        ref = strip_v.at[i % 2, :, pl.ds(0, depth)]
        pltpu.make_async_copy(ref, ref, strip_sem.at[i % 2]).wait()

    def load(c, slot, k, src):
        return pltpu.make_async_copy(src, b_v.at[slot, pl.ds(k * n, n), :], load_sem.at[slot, k])

    def own_rows(r, c, slot):
        for i in range(TILES):
            strip_wait(r, i)
            if i + 1 < TILES:
                strip_start(r, i + 1)
            else:
                @pl.when(c + 1 < chunks)
                def _():
                    strip_start(r, 0)
            depth = r * n + (i + 1) * rt
            acc = jnp.dot(
                strip_v[i % 2, :, :depth], b_v[slot, :depth, :], preferred_element_type=jnp.float32
            )
            out = pltpu.make_async_copy(xo_v.at[i % 2], x_tile(i, c), out_sem.at[i % 2])
            if i >= 2:
                out.wait()
            else:
                @pl.when(c > 0)
                def _(out=out):
                    out.wait()
            xo_v[i % 2] = acc.astype(xo_v.dtype)
            out.start()

    def own_rows_drain():
        for s in range(2):
            pltpu.make_async_copy(xo_v.at[s], x_tile(s, 0), out_sem.at[s]).wait()

    def simple_rows(r, prior):
        def loads(c, slot):
            return [load(c, slot, k, ref(c)) for k, ref in prior]

        for cp in loads(0, 0):
            cp.start()
        strip_start(r, 0)

        def step(c, carry):
            slot = lax.rem(c, 2)
            for cp in loads(c, slot):
                cp.wait()

            @pl.when(c + 1 < chunks)
            def _():
                for cp in loads(c + 1, 1 - slot):
                    cp.start()

            own_rows(r, c, slot)
            return carry

        lax.fori_loop(0, chunks, step, 0)
        own_rows_drain()

    @pl.when(row == 0)
    def _():
        def send(c, carry):
            remote(own_chunk(c), rb_ref.at[0, c], b_tx, b0_rx.at[c], 1, col).start()
            return carry

        lax.fori_loop(0, chunks, send, 0)
        l_exchange_start()
        l_forward()
        l_exchange_end()
        simple_rows(0, [(0, own_chunk)])
        l_exchange_drain()
        arrived(b_ref, b_tx)

    @pl.when(row == 1)
    def _():
        l_exchange_start()

        def send_own(c, carry):
            remote(own_chunk(c), rb_ref.at[1, c], b_tx, b1_rx.at[c], 2, col).start()
            return carry

        def forward(c, carry):
            blk = rb_ref.at[0, c]
            arrived(blk, b0_rx.at[c])
            remote(blk, blk, fwd_tx, b0_rx.at[c], 2, col).start()
            return carry

        lax.fori_loop(0, chunks, send_own, 0)
        lax.fori_loop(0, chunks, forward, 0)
        l_forward()
        l_exchange_end()
        simple_rows(1, [(0, lambda c: rb_ref.at[0, c]), (1, own_chunk)])
        l_exchange_drain()
        arrived(b_ref, b_tx)
        arrived(rb_ref.at[0], fwd_tx)

    @pl.when(row == 2)
    def _():
        l_exchange_start()
        lo, hi = pl.ds(0, half), pl.ds(half, half)

        def own(p):
            return lg_ref.at[1, col, p]

        def other(p):
            return lg_ref.at[1, y_peer, p]

        arrived(own(lo), l3_rx.at[0])
        remote(own(lo), own(lo), l3_tx.at[0], l3_rx.at[2], row, y_peer).start()
        remote(own(lo), own(lo), l3_tx.at[1], l3_rx.at[4], row, core_peer).start()
        arrived(own(hi), l3_rx.at[1])
        remote(own(hi), own(hi), l3_tx.at[2], l3_rx.at[5], row, core_peer).start()
        l_forward()
        arrived(other(lo), l3_rx.at[2])
        remote(other(lo), other(lo), l3_tx.at[3], l3_rx.at[6], row, core_peer).start()
        arrived(other(hi), l3_rx.at[3])
        remote(other(hi), other(hi), l3_tx.at[4], l3_rx.at[7], row, core_peer).start()
        l_exchange_end()
        for s, (blk, p) in enumerate(((core_peer, lo), (core_peer, hi), (far, lo), (far, hi))):
            arrived(lg_ref.at[1, blk, p], l3_rx.at[4 + s])
        for k in range(4):
            pltpu.make_async_copy(lg_ref.at[1, k], l3_v.at[:, pl.ds(k * n, n)], l3_sem).start()

        def early(c, slot):
            return [
                load(c, slot, 1, rb_ref.at[1, c]), load(c, slot, 2, own_chunk(c)), load(c, slot, 3, rb_ref.at[2, c])
            ]

        def prefetch(c, slot):
            arrived(rb_ref.at[1, c], b1_rx.at[c])
            arrived(rb_ref.at[2, c], b3_rx.at[c])
            for cp in early(c, slot):
                cp.start()

        def x3_send(i, c, slot):
            return remote(x3_v.at[slot, i], x_tile(i, c), x3_tx.at[slot, i], x3_rx, 3, col)

        prefetch(0, 0)
        strip_start(2, 0)
        pltpu.make_async_copy(l3_v, l3_v, l3_sem).wait()

        def step(c, carry):
            slot = lax.rem(c, 2)
            arrived(rb_ref.at[0, c], b0_rx.at[c])
            last = load(c, slot, 0, rb_ref.at[0, c])
            last.start()
            for cp in early(c, slot):
                cp.wait()
            last.wait()
            for i in range(TILES):
                @pl.when(c >= 2)
                def _(i=i):
                    x3_send(i, c, slot).wait_send()

                depth = 3 * n + (i + 1) * rt
                acc = jnp.dot(
                    l3_v[pl.ds(i * rt, rt), :depth], b_v[slot, :depth, :], preferred_element_type=jnp.float32
                )
                x3_v[slot, i] = acc.astype(x3_v.dtype)
                if i:
                    x3_send(i - 1, c, slot).start()

            @pl.when(c + 1 < chunks)
            def _():
                prefetch(c + 1, 1 - slot)

            x3_send(TILES - 1, c, slot).start()
            own_rows(2, c, slot)
            return carry

        lax.fori_loop(0, chunks, step, 0)
        own_rows_drain()
        for slot in range(2):
            for i in range(TILES):
                x3_send(i, 0, slot).wait_send()
        l_exchange_drain()
        for s in range(5):
            arrived(own(lo), l3_tx.at[s])

    @pl.when(row == 3)
    def _():
        lo, hi = pl.ds(0, half), pl.ds(half, half)
        for s, p in enumerate((lo, hi)):
            remote(l_ref.at[p], lg_ref.at[1, col, p], l3_tx.at[s], l3_rx.at[s], 2, col).start()
        remote(l_ref.at[hi], lg_ref.at[1, col, hi], l3_tx.at[2], cross_rx, row, y_peer).start()
        blk = lg_ref.at[1, y_peer, hi]
        arrived(blk, cross_rx)
        remote(blk, blk, l3_tx.at[3], l3_rx.at[3], 2, col).start()

        def send(c, carry):
            remote(own_chunk(c), rb_ref.at[2, c], b_tx, b3_rx.at[c], 2, col).start()
            return carry

        lax.fori_loop(0, chunks, send, 0)
        for s in range(4):
            arrived(blk, l3_tx.at[s])
        arrived(b_ref, b_tx)
        arrived(x_ref, x3_rx)


def solution(mesh):
    block_spec = P(("batch", "row"), "col")

    def local_product(l_block, b_block):
        n, m = b_block.shape
        rt = n // TILES
        chunks = m // CHUNK
        dma = pltpu.SemaphoreType.DMA
        hbm = pl.BlockSpec(memory_space=pl.ANY)
        x, _, _ = pl.pallas_call(
            kernel,
            out_shape=(
                jax.ShapeDtypeStruct((n, m), b_block.dtype),
                jax.ShapeDtypeStruct((3, chunks, n, CHUNK), b_block.dtype),
                jax.ShapeDtypeStruct((2, 4, n, n), l_block.dtype),
            ),
            in_specs=[hbm, hbm],
            out_specs=(hbm, hbm, hbm),
            scratch_shapes=[
                pltpu.VMEM((n, 4 * n), l_block.dtype),
                pltpu.VMEM((2, 4 * n, CHUNK), b_block.dtype),
                pltpu.VMEM((2, rt, 3 * n), l_block.dtype),
                pltpu.VMEM((2, TILES, rt, CHUNK), b_block.dtype),
                pltpu.VMEM((2, rt, CHUNK), b_block.dtype),
                dma((chunks,)), dma((chunks,)), dma((chunks,)), dma((3,)), dma((8,)), dma, dma,
                dma, dma, dma((3,)), dma((5,)), dma((2, TILES)),
                dma((2, 4)), dma((2,)), dma((2,)), dma,
            ],
            compiler_params=pltpu.CompilerParams(has_side_effects=True, vmem_limit_bytes=66 * 1000 * 1000),
        )(l_block, b_block)
        return x

    return jax.shard_map(
        local_product, mesh=mesh, in_specs=(block_spec, block_spec), out_specs=block_spec, check_vma=False
    )
```

```python
import functools

import jax
import jax.numpy as jnp
from jax import lax
from jax.experimental import pallas as pl
from jax.experimental.pallas import tpu as pltpu
from jax.sharding import PartitionSpec as P

MESH = pl.DeviceIdType.MESH
TILES = 4
CHUNK = 256


def mid_order(chunks):
    return [(1, c) for c in range(chunks)] + [(0, c) for c in range(chunks)]


def kernel(
    l_ref, b_ref, x_ref, rb_ref, lg_ref,
    l3_v, b_v, strip_v, x3_v, xo_v,
    b0_rx, b1_rx, b3_rx, l_rx, l3_rx, cross_rx, x3_rx,
    b_tx, fwd_tx, l_tx, l3_tx, x3_tx,
    load_sem, strip_sem, out_sem, l3_sem,
):
    n, m = b_ref.shape
    half = n // 2
    rt = n // TILES
    w = CHUNK
    chunks = m // w
    batch, row, col = (lax.axis_index(a) for a in ("batch", "row", "col"))
    core_peer = col + 1 - 2 * lax.rem(col, 2)
    y_peer = lax.rem(col + 2, 4)
    far = lax.rem(core_peer + 2, 4)

    def remote(src, dst, send, recv, r, c):
        return pltpu.make_async_remote_copy(
            src_ref=src, dst_ref=dst, send_sem=send, recv_sem=recv,
            device_id=(batch, r, c), device_id_type=MESH,
        )

    def arrived(dst, sem):
        pltpu.make_async_copy(dst, dst, sem).wait()

    def own_chunk(c):
        return b_ref.at[:, pl.ds(pl.multiple_of(c * w, w), w)]

    def x_tile(i, c):
        return x_ref.at[pl.ds(pl.multiple_of(i * rt, rt), rt), pl.ds(pl.multiple_of(c * w, w), w)]

    def l_exchange_start():
        remote(l_ref, lg_ref.at[0, col], l_tx.at[0], l_rx.at[0], row, y_peer).start()
        remote(l_ref, lg_ref.at[0, col], l_tx.at[1], l_rx.at[1], row, core_peer).start()

    def l_forward():
        blk = lg_ref.at[0, y_peer]
        arrived(blk, l_rx.at[0])
        remote(blk, blk, l_tx.at[2], l_rx.at[2], row, core_peer).start()

    def l_exchange_end():
        arrived(lg_ref.at[0, core_peer], l_rx.at[1])
        arrived(lg_ref.at[0, far], l_rx.at[2])

    def l_exchange_drain():
        for s in range(3):
            arrived(l_ref, l_tx.at[s])

    def strip_start(r, i):
        slot = lax.rem(i, 2)
        rows = pl.ds(pl.multiple_of(i * rt, rt), rt)
        for k in range(r + 1):
            dst = strip_v.at[slot, :, pl.ds(k * n, n)]

            @pl.when(col == k)
            def _(dst=dst):
                pltpu.make_async_copy(l_ref.at[rows], dst, strip_sem.at[slot]).start()

            @pl.when(col != k)
            def _(dst=dst, k=k):
                pltpu.make_async_copy(lg_ref.at[0, k, rows], dst, strip_sem.at[slot]).start()

    def strip_wait(r, i):
        slot = lax.rem(i, 2)
        ref = strip_v.at[slot, :, pl.ds(0, (r + 1) * n)]
        pltpu.make_async_copy(ref, ref, strip_sem.at[slot]).wait()

    def load(c, slot, k, src):
        return pltpu.make_async_copy(src, b_v.at[slot, pl.ds(k * n, n), :], load_sem.at[slot, k])

    def own_rows(r, c, slot):
        depth = (r + 1) * n

        def tile(i, carry):
            part = lax.rem(i, 2)
            strip_wait(r, i)

            @pl.when((i + 1 < TILES) | (c + 1 < chunks))
            def _():
                strip_start(r, lax.rem(i + 1, TILES))

            out = pltpu.make_async_copy(xo_v.at[part], x_tile(i, c), out_sem.at[part])

            @pl.when((i >= 2) | (c > 0))
            def _():
                out.wait()

            xo_v[part] = jnp.dot(
                strip_v[part, :, :depth], b_v[slot, :depth, :], preferred_element_type=jnp.float32
            ).astype(xo_v.dtype)
            out.start()
            return carry

        lax.fori_loop(0, TILES, tile, 0)

    def own_rows_drain():
        for s in range(2):
            pltpu.make_async_copy(xo_v.at[s], x_tile(s, 0), out_sem.at[s]).wait()

    def simple_rows(r, prior):
        def loads(c, slot):
            return [load(c, slot, k, ref(c)) for k, ref in prior]

        for cp in loads(0, 0):
            cp.start()
        strip_start(r, 0)

        def step(c, carry):
            slot = lax.rem(c, 2)
            for cp in loads(c, slot):
                cp.wait()

            @pl.when(c + 1 < chunks)
            def _():
                for cp in loads(c + 1, 1 - slot):
                    cp.start()

            own_rows(r, c, slot)
            return carry

        lax.fori_loop(0, chunks, step, 0)
        own_rows_drain()

    @pl.when(row == 0)
    def _():
        def send(c, carry):
            remote(own_chunk(c), rb_ref.at[0, c], b_tx, b0_rx.at[c], 1, col).start()
            return carry

        lax.fori_loop(0, chunks, send, 0)
        l_exchange_start()
        l_forward()
        l_exchange_end()
        simple_rows(0, [(0, own_chunk)])
        l_exchange_drain()
        arrived(b_ref, b_tx)

    @pl.when(row == 1)
    def _():
        l_exchange_start()

        def send_own(c, carry):
            remote(own_chunk(c), rb_ref.at[1, c], b_tx, b1_rx.at[c], 2, col).start()
            return carry

        def forward(c, carry):
            blk = rb_ref.at[0, c]
            arrived(blk, b0_rx.at[c])
            remote(blk, blk, fwd_tx, b0_rx.at[c], 2, col).start()
            return carry

        lax.fori_loop(0, chunks, send_own, 0)
        lax.fori_loop(0, chunks, forward, 0)
        l_forward()
        l_exchange_end()
        simple_rows(1, [(0, lambda c: rb_ref.at[0, c]), (1, own_chunk)])
        l_exchange_drain()
        arrived(b_ref, b_tx)
        arrived(rb_ref.at[0], fwd_tx)

    @pl.when(row == 2)
    def _():
        l_exchange_start()
        lo, hi = pl.ds(0, half), pl.ds(half, half)

        def own(p):
            return lg_ref.at[1, col, p]

        def other(p):
            return lg_ref.at[1, y_peer, p]

        arrived(own(lo), l3_rx.at[0])
        remote(own(lo), own(lo), l3_tx.at[0], l3_rx.at[2], row, y_peer).start()
        remote(own(lo), own(lo), l3_tx.at[1], l3_rx.at[4], row, core_peer).start()
        arrived(own(hi), l3_rx.at[1])
        remote(own(hi), own(hi), l3_tx.at[2], l3_rx.at[5], row, core_peer).start()
        l_forward()
        arrived(other(lo), l3_rx.at[2])
        remote(other(lo), other(lo), l3_tx.at[3], l3_rx.at[6], row, core_peer).start()
        arrived(other(hi), l3_rx.at[3])
        remote(other(hi), other(hi), l3_tx.at[4], l3_rx.at[7], row, core_peer).start()
        l_exchange_end()
        for s, (blk, p) in enumerate(((core_peer, lo), (core_peer, hi), (far, lo), (far, hi))):
            arrived(lg_ref.at[1, blk, p], l3_rx.at[4 + s])
        for k in range(4):
            pltpu.make_async_copy(lg_ref.at[1, k], l3_v.at[:, pl.ds(k * n, n)], l3_sem).start()

        def early(c, slot):
            return [
                load(c, slot, 1, rb_ref.at[1, c]), load(c, slot, 2, own_chunk(c)), load(c, slot, 3, rb_ref.at[2, c])
            ]

        def prefetch(c, slot):
            arrived(rb_ref.at[1, c], b1_rx.at[c])
            arrived(rb_ref.at[2, c], b3_rx.at[c])
            for cp in early(c, slot):
                cp.start()

        def x3_send(i, c, slot):
            return remote(x3_v.at[slot, i], x_tile(i, c), x3_tx.at[slot, i], x3_rx, 3, col)

        prefetch(0, 0)
        strip_start(2, 0)
        pltpu.make_async_copy(l3_v, l3_v, l3_sem).wait()

        def step(c, carry):
            slot = lax.rem(c, 2)
            arrived(rb_ref.at[0, c], b0_rx.at[c])
            last = load(c, slot, 0, rb_ref.at[0, c])
            last.start()
            for cp in early(c, slot):
                cp.wait()
            last.wait()
            def tile(i, inner):
                @pl.when(c >= 2)
                def _():
                    x3_send(i, c, slot).wait_send()

                rows = pl.ds(pl.multiple_of(i * rt, rt), rt)
                x3_v[slot, i] = jnp.dot(
                    l3_v[rows, :], b_v[slot], preferred_element_type=jnp.float32
                ).astype(x3_v.dtype)

                @pl.when(i > 0)
                def _():
                    x3_send(i - 1, c, slot).start()

                return inner

            lax.fori_loop(0, TILES, tile, 0)

            @pl.when(c + 1 < chunks)
            def _():
                prefetch(c + 1, 1 - slot)

            x3_send(TILES - 1, c, slot).start()
            own_rows(2, c, slot)
            return carry

        lax.fori_loop(0, chunks, step, 0)
        own_rows_drain()
        for slot in range(2):
            for i in range(TILES):
                x3_send(i, 0, slot).wait_send()
        l_exchange_drain()
        for s in range(5):
            arrived(own(lo), l3_tx.at[s])

    @pl.when(row == 3)
    def _():
        lo, hi = pl.ds(0, half), pl.ds(half, half)
        for s, p in enumerate((lo, hi)):
            remote(l_ref.at[p], lg_ref.at[1, col, p], l3_tx.at[s], l3_rx.at[s], 2, col).start()
        remote(l_ref.at[hi], lg_ref.at[1, col, hi], l3_tx.at[2], cross_rx, row, y_peer).start()
        blk = lg_ref.at[1, y_peer, hi]
        arrived(blk, cross_rx)
        remote(blk, blk, l3_tx.at[3], l3_rx.at[3], 2, col).start()

        def send(c, carry):
            remote(own_chunk(c), rb_ref.at[2, c], b_tx, b3_rx.at[c], 2, col).start()
            return carry

        lax.fori_loop(0, chunks, send, 0)
        for s in range(4):
            arrived(blk, l3_tx.at[s])
        arrived(b_ref, b_tx)
        arrived(x_ref, x3_rx)


def solution(mesh):
    block_spec = P(("batch", "row"), "col")

    def local_product(l_block, b_block):
        n, m = b_block.shape
        rt = n // TILES
        chunks = m // CHUNK
        dma = pltpu.SemaphoreType.DMA
        hbm = pl.BlockSpec(memory_space=pl.ANY)
        x, _, _ = pl.pallas_call(
            kernel,
            out_shape=(
                jax.ShapeDtypeStruct((n, m), b_block.dtype),
                jax.ShapeDtypeStruct((3, chunks, n, CHUNK), b_block.dtype),
                jax.ShapeDtypeStruct((2, 4, n, n), l_block.dtype),
            ),
            in_specs=[hbm, hbm],
            out_specs=(hbm, hbm, hbm),
            scratch_shapes=[
                pltpu.VMEM((n, 4 * n), l_block.dtype),
                pltpu.VMEM((2, 4 * n, CHUNK), b_block.dtype),
                pltpu.VMEM((2, rt, 3 * n), l_block.dtype),
                pltpu.VMEM((2, TILES, rt, CHUNK), b_block.dtype),
                pltpu.VMEM((2, rt, CHUNK), b_block.dtype),
                dma((chunks,)), dma((chunks,)), dma((chunks,)), dma((3,)), dma((8,)), dma, dma,
                dma, dma, dma((3,)), dma((5,)), dma((2, TILES)),
                dma((2, 4)), dma((2,)), dma((2,)), dma,
            ],
            compiler_params=pltpu.CompilerParams(has_side_effects=True, vmem_limit_bytes=66 * 1000 * 1000),
        )(l_block, b_block)
        return x

    return jax.shard_map(
        local_product, mesh=mesh, in_specs=(block_spec, block_spec), out_specs=block_spec, check_vma=False
    )
```

```python
import functools

import jax
import jax.numpy as jnp
from jax import lax
from jax.experimental import pallas as pl
from jax.experimental.pallas import tpu as pltpu
from jax.sharding import PartitionSpec as P

MESH = pl.DeviceIdType.MESH
TILES = 4
CHUNK = 256


def mid_order(chunks):
    first = chunks * 3 // 4
    late = list(range(first, chunks - 2))
    gap = -(-(chunks - 2) // (len(late) + 1))
    order = [(1, c) for c in range(first)]
    for c in range(chunks - 2):
        order.append((0, c))
        if late and (c + 1) % gap == 0:
            order.append((1, late.pop(0)))
    assert not late
    return order + [(k, c) for c in (chunks - 2, chunks - 1) for k in (1, 0)]


def kernel(
    l_ref, b_ref, x_ref, rb_ref, lg_ref,
    l3_v, b_v, strip_v, x3_v, xo_v, p3_v, p2_v,
    b0_rx, b1_rx, b3_rx, l_rx, l3_rx, cross_rx, x3_rx,
    b_tx, fwd_tx, l_tx, l3_tx, x3_tx,
    load_sem, strip_sem, out_sem, l3_sem, piece_sem,
):
    n, m = b_ref.shape
    half = n // 2
    rt = n // TILES
    w = CHUNK
    chunks = m // w
    edge, hw = chunks - 1, w // 2
    batch, row, col = (lax.axis_index(a) for a in ("batch", "row", "col"))
    core_peer = col + 1 - 2 * lax.rem(col, 2)
    y_peer = lax.rem(col + 2, 4)
    far = lax.rem(core_peer + 2, 4)

    def remote(src, dst, send, recv, r, c):
        return pltpu.make_async_remote_copy(
            src_ref=src, dst_ref=dst, send_sem=send, recv_sem=recv,
            device_id=(batch, r, c), device_id_type=MESH,
        )

    def arrived(dst, sem):
        pltpu.make_async_copy(dst, dst, sem).wait()

    def own_chunk(c):
        return b_ref.at[:, pl.ds(pl.multiple_of(c * w, w), w)]

    def x_tile(i, c):
        return x_ref.at[pl.ds(pl.multiple_of(i * rt, rt), rt), pl.ds(pl.multiple_of(c * w, w), w)]

    def l_exchange_start():
        remote(l_ref, lg_ref.at[0, col], l_tx.at[0], l_rx.at[0], row, y_peer).start()
        remote(l_ref, lg_ref.at[0, col], l_tx.at[1], l_rx.at[1], row, core_peer).start()

    def l_forward():
        blk = lg_ref.at[0, y_peer]
        arrived(blk, l_rx.at[0])
        remote(blk, blk, l_tx.at[2], l_rx.at[2], row, core_peer).start()

    def l_exchange_end():
        arrived(lg_ref.at[0, core_peer], l_rx.at[1])
        arrived(lg_ref.at[0, far], l_rx.at[2])

    def l_exchange_drain():
        for s in range(3):
            arrived(l_ref, l_tx.at[s])

    def strip_start(r, i):
        slot = lax.rem(i, 2)
        rows = pl.ds(pl.multiple_of(i * rt, rt), rt)
        for k in range(r + 1):
            dst = strip_v.at[slot, :, pl.ds(k * n, n)]

            @pl.when(col == k)
            def _(dst=dst):
                pltpu.make_async_copy(l_ref.at[rows], dst, strip_sem.at[slot]).start()

            @pl.when(col != k)
            def _(dst=dst, k=k):
                pltpu.make_async_copy(lg_ref.at[0, k, rows], dst, strip_sem.at[slot]).start()

    def strip_wait(r, i):
        slot = lax.rem(i, 2)
        ref = strip_v.at[slot, :, pl.ds(0, (r + 1) * n)]
        pltpu.make_async_copy(ref, ref, strip_sem.at[slot]).wait()

    def load(c, slot, k, src):
        return pltpu.make_async_copy(src, b_v.at[slot, pl.ds(k * n, n), :], load_sem.at[slot, k])

    def own_rows(r, c, slot, end):
        depth = (r + 1) * n

        def tile(i, carry):
            part = lax.rem(i, 2)
            strip_wait(r, i)

            @pl.when((i + 1 < TILES) | (c + 1 < end))
            def _():
                strip_start(r, lax.rem(i + 1, TILES))

            out = pltpu.make_async_copy(xo_v.at[part], x_tile(i, c), out_sem.at[part])

            @pl.when((i >= 2) | (c > 0))
            def _():
                out.wait()

            xo_v[part] = jnp.dot(
                strip_v[part, :, :depth], b_v[slot, :depth, :], preferred_element_type=jnp.float32
            ).astype(xo_v.dtype)
            out.start()
            return carry

        lax.fori_loop(0, TILES, tile, 0)

    def own_rows_drain():
        for s in range(2):
            pltpu.make_async_copy(xo_v.at[s], x_tile(s, 0), out_sem.at[s]).wait()

    def simple_rows(r, prior):
        def loads(c, slot):
            return [load(c, slot, k, ref(c)) for k, ref in prior]

        for cp in loads(0, 0):
            cp.start()
        strip_start(r, 0)

        def step(c, carry):
            slot = lax.rem(c, 2)
            for cp in loads(c, slot):
                cp.wait()

            @pl.when(c + 1 < chunks)
            def _():
                for cp in loads(c + 1, 1 - slot):
                    cp.start()

            own_rows(r, c, slot, chunks)
            return carry

        lax.fori_loop(0, chunks, step, 0)
        own_rows_drain()

    @pl.when(row == 0)
    def _():
        def send(c, carry):
            remote(own_chunk(c), rb_ref.at[0, c], b_tx, b0_rx.at[c], 1, col).start()
            return carry

        lax.fori_loop(0, chunks, send, 0)
        l_exchange_start()
        l_forward()
        l_exchange_end()
        simple_rows(0, [(0, own_chunk)])
        l_exchange_drain()
        arrived(b_ref, b_tx)

    @pl.when(row == 1)
    def _():
        l_exchange_start()

        for k, c in mid_order(chunks):
            blk = rb_ref.at[k, c]
            if k == 1:
                remote(own_chunk(c), blk, b_tx, b1_rx.at[c], 2, col).start()
                continue
            arrived(blk, b0_rx.at[c])
            if c < edge:
                remote(blk, blk, fwd_tx, b0_rx.at[c], 2, col).start()
                continue
            for h in range(2):
                part = blk.at[:, pl.ds(h * hw, hw)]
                remote(part, part, fwd_tx, b0_rx.at[c + h], 2, col).start()
        l_forward()
        l_exchange_end()
        simple_rows(1, [(0, lambda c: rb_ref.at[0, c]), (1, own_chunk)])
        l_exchange_drain()
        arrived(b_ref, b_tx)
        arrived(rb_ref.at[0], fwd_tx)

    @pl.when(row == 2)
    def _():
        l_exchange_start()
        lo, hi = pl.ds(0, half), pl.ds(half, half)

        def own(p):
            return lg_ref.at[1, col, p]

        def other(p):
            return lg_ref.at[1, y_peer, p]

        arrived(own(lo), l3_rx.at[0])
        remote(own(lo), own(lo), l3_tx.at[0], l3_rx.at[2], row, y_peer).start()
        remote(own(lo), own(lo), l3_tx.at[1], l3_rx.at[4], row, core_peer).start()
        arrived(own(hi), l3_rx.at[1])
        remote(own(hi), own(hi), l3_tx.at[2], l3_rx.at[5], row, core_peer).start()
        l_forward()
        arrived(other(lo), l3_rx.at[2])
        remote(other(lo), other(lo), l3_tx.at[3], l3_rx.at[6], row, core_peer).start()
        arrived(other(hi), l3_rx.at[3])
        remote(other(hi), other(hi), l3_tx.at[4], l3_rx.at[7], row, core_peer).start()
        l_exchange_end()
        for s, (blk, p) in enumerate(((core_peer, lo), (core_peer, hi), (far, lo), (far, hi))):
            arrived(lg_ref.at[1, blk, p], l3_rx.at[4 + s])
        for k in range(4):
            pltpu.make_async_copy(lg_ref.at[1, k], l3_v.at[:, pl.ds(k * n, n)], l3_sem).start()

        def load1(c, slot):
            return load(c, slot, 1, rb_ref.at[1, c])

        def load23(c, slot):
            return load(c, slot, 2, own_chunk(c)), load(c, slot, 3, rb_ref.at[2, c])

        def prefetch23(c, slot):
            arrived(rb_ref.at[2, c], b3_rx.at[c])
            for cp in load23(c, slot):
                cp.start()

        def prefetch1(c, slot):
            arrived(rb_ref.at[1, c], b1_rx.at[c])
            load1(c, slot).start()

        def x3_send(i, c, slot):
            return remote(x3_v.at[slot, i], x_tile(i, c), x3_tx.at[slot, i], x3_rx, 3, col)

        prefetch23(0, 0)
        prefetch1(0, 0)
        strip_start(2, 0)
        pltpu.make_async_copy(l3_v, l3_v, l3_sem).wait()

        e_slot, e_spare = edge % 2, 1 - edge % 2

        def piece(s):
            q = lax.rem(s, 6)
            return strip_v.at[q // 3, :, pl.ds(pl.multiple_of(lax.rem(q, 3) * n, n), n)]

        def piece_start(s):
            k, i = 2 - s // TILES, s % TILES
            rows = pl.ds(i * rt, rt)

            @pl.when(col == k)
            def _():
                pltpu.make_async_copy(l_ref.at[rows], piece(s), piece_sem.at[s]).start()

            @pl.when(col != k)
            def _():
                pltpu.make_async_copy(lg_ref.at[0, k, rows], piece(s), piece_sem.at[s]).start()

        def piece_wait(s):
            arrived(piece(s), piece_sem.at[s])

        def tile_rows(i):
            return pl.ds(pl.multiple_of(i * rt, rt), rt)

        def dot(a, b):
            return jnp.dot(a, b, preferred_element_type=jnp.float32)

        def terms23():
            for s in range(TILES):
                piece_start(s)
            prefetch23(edge, e_slot)
            for cp in load23(edge, e_slot):
                cp.wait()

            def tile(i, carry):
                rows = tile_rows(i)
                p3_v[rows, :] = dot(l3_v[rows, 2 * n :], b_v[e_slot, 2 * n :, :])
                piece_wait(i)
                p2_v[rows, :] = dot(piece(i)[...], b_v[e_slot, 2 * n : 3 * n, :])
                return carry

            lax.fori_loop(0, TILES, tile, 0)
            prefetch1(edge - 1, e_spare)
            strip_start(2, 0)

        def step(c, carry):
            slot = lax.rem(c, 2)
            pl.when(c == edge - 1)(terms23)
            arrived(rb_ref.at[0, c], b0_rx.at[c])
            last = load(c, slot, 0, rb_ref.at[0, c])
            last.start()
            for cp in (load1(c, slot), *load23(c, slot), last):
                cp.wait()
            def tile(i, inner):
                @pl.when(c >= 2)
                def _():
                    x3_send(i, c, slot).wait_send()

                rows = pl.ds(pl.multiple_of(i * rt, rt), rt)
                x3_v[slot, i] = jnp.dot(
                    l3_v[rows, :], b_v[slot], preferred_element_type=jnp.float32
                ).astype(x3_v.dtype)

                @pl.when(i > 0)
                def _():
                    x3_send(i - 1, c, slot).start()

                return inner

            lax.fori_loop(0, TILES, tile, 0)

            x3_send(TILES - 1, c, slot).start()

            @pl.when(c + 1 < edge)
            def _():
                prefetch23(c + 1, 1 - slot)

            @pl.when(c + 2 < edge)
            def _():
                prefetch1(c + 1, 1 - slot)

            own_rows(2, c, slot, edge - 1)
            return carry

        lax.fori_loop(0, edge, step, 0)
        own_rows_drain()

        for s in range(TILES, TILES + 6):
            piece_start(s)
        prefetch1(edge, e_slot)
        load1(edge, e_slot).wait()

        def terms1(i, carry):
            rows = tile_rows(i)
            p3_v[rows, :] += dot(l3_v[rows, n : 2 * n], b_v[e_slot, n : 2 * n, :])
            piece_wait(TILES + i)
            p2_v[rows, :] += dot(piece(TILES + i)[...], b_v[e_slot, n : 2 * n, :])
            return carry

        lax.fori_loop(0, TILES, terms1, 0)
        for s in range(10, 12):
            piece_start(s)
        for s in range(2):
            for i in range(TILES):
                x3_send(i, 0, s).wait_send()

        def half_lanes(h):
            return pl.ds(pl.multiple_of(h * hw, hw), hw)

        def half_tile(i, h):
            return x_ref.at[tile_rows(i), pl.ds(pl.multiple_of(edge * w + h * hw, hw), hw)]

        def x3_half(i, h):
            return remote(
                x3_v.at[e_slot, i, :, half_lanes(h)], half_tile(i, h), x3_tx.at[e_slot, i], x3_rx, 3, col
            )

        def x2_half(i, h):
            return pltpu.make_async_copy(
                x3_v.at[e_spare, i, :, half_lanes(h)], half_tile(i, h), x3_tx.at[e_spare, i]
            )

        def half_step(h, carry):
            lanes = half_lanes(h)
            part = rb_ref.at[0, edge, :, lanes]
            arrived(part, b0_rx.at[edge + h])
            last = pltpu.make_async_copy(part, b_v.at[e_slot, pl.ds(0, n), lanes], load_sem.at[e_slot, 0])
            last.start()
            last.wait()

            def tile3(i, inner):
                rows = tile_rows(i)
                x3_v[e_slot, i, :, lanes] = (
                    p3_v[rows, lanes] + dot(l3_v[rows, :n], b_v[e_slot, :n, lanes])
                ).astype(x3_v.dtype)

                @pl.when(i > 0)
                def _():
                    x3_half(i - 1, h).start()

                return inner

            def tile2(i, inner):
                @pl.when(h == 0)
                def _():
                    piece_wait(2 * TILES + i)

                x3_v[e_spare, i, :, lanes] = (
                    p2_v[tile_rows(i), lanes] + dot(piece(2 * TILES + i)[...], b_v[e_slot, :n, lanes])
                ).astype(x3_v.dtype)

                @pl.when(i == 0)
                def _():
                    x3_half(TILES - 1, h).start()

                @pl.when(i > 0)
                def _():
                    x2_half(i - 1, h).start()

                return inner

            lax.fori_loop(0, TILES, tile3, 0)
            lax.fori_loop(0, TILES, tile2, 0)
            x2_half(TILES - 1, h).start()
            return carry

        lax.fori_loop(0, 2, half_step, 0)
        for s in range(2):
            for i in range(TILES):
                arrived(x3_v.at[s, i], x3_tx.at[s, i])
        l_exchange_drain()
        for s in range(5):
            arrived(own(lo), l3_tx.at[s])

    @pl.when(row == 3)
    def _():
        lo, hi = pl.ds(0, half), pl.ds(half, half)
        for s, p in enumerate((lo, hi)):
            remote(l_ref.at[p], lg_ref.at[1, col, p], l3_tx.at[s], l3_rx.at[s], 2, col).start()
        remote(l_ref.at[hi], lg_ref.at[1, col, hi], l3_tx.at[2], cross_rx, row, y_peer).start()
        blk = lg_ref.at[1, y_peer, hi]
        arrived(blk, cross_rx)
        remote(blk, blk, l3_tx.at[3], l3_rx.at[3], 2, col).start()

        def send(c, carry):
            remote(own_chunk(c), rb_ref.at[2, c], b_tx, b3_rx.at[c], 2, col).start()
            return carry

        lax.fori_loop(0, chunks, send, 0)
        for s in range(4):
            arrived(blk, l3_tx.at[s])
        arrived(b_ref, b_tx)
        arrived(x_ref, x3_rx)


def solution(mesh):
    block_spec = P(("batch", "row"), "col")

    def local_product(l_block, b_block):
        n, m = b_block.shape
        rt = n // TILES
        chunks = m // CHUNK
        dma = pltpu.SemaphoreType.DMA
        hbm = pl.BlockSpec(memory_space=pl.ANY)
        x, _, _ = pl.pallas_call(
            kernel,
            out_shape=(
                jax.ShapeDtypeStruct((n, m), b_block.dtype),
                jax.ShapeDtypeStruct((3, chunks, n, CHUNK), b_block.dtype),
                jax.ShapeDtypeStruct((2, 4, n, n), l_block.dtype),
            ),
            in_specs=[hbm, hbm],
            out_specs=(hbm, hbm, hbm),
            scratch_shapes=[
                pltpu.VMEM((n, 4 * n), l_block.dtype),
                pltpu.VMEM((2, 4 * n, CHUNK), b_block.dtype),
                pltpu.VMEM((2, rt, 3 * n), l_block.dtype),
                pltpu.VMEM((2, TILES, rt, CHUNK), b_block.dtype),
                pltpu.VMEM((2, rt, CHUNK), b_block.dtype),
                pltpu.VMEM((n, CHUNK), jnp.float32),
                pltpu.VMEM((n, CHUNK), jnp.float32),
                dma((chunks + 1,)), dma((chunks,)), dma((chunks,)), dma((3,)), dma((8,)), dma, dma,
                dma, dma, dma((3,)), dma((5,)), dma((2, TILES)),
                dma((2, 4)), dma((2,)), dma((2,)), dma, dma((12,)),
            ],
            compiler_params=pltpu.CompilerParams(has_side_effects=True, vmem_limit_bytes=66 * 1000 * 1000),
        )(l_block, b_block)
        return x

    return jax.shard_map(
        local_product, mesh=mesh, in_specs=(block_spec, block_spec), out_specs=block_spec, check_vma=False
    )
```

```python
import functools

import jax
import jax.numpy as jnp
from jax import lax
from jax.experimental import pallas as pl
from jax.experimental.pallas import tpu as pltpu
from jax.sharding import PartitionSpec as P

MESH = pl.DeviceIdType.MESH
PARTS = 8
TILES = 4
CHUNK = 256


def mid_order(chunks):
    first = chunks * 3 // 4
    late = list(range(first, chunks - 2))
    gap = -(-(chunks - 2) // (len(late) + 1))
    order = [(1, c) for c in range(first)]
    for c in range(chunks - 2):
        order.append((0, c))
        if late and (c + 1) % gap == 0:
            order.append((1, late.pop(0)))
    assert not late
    return order + [(k, c) for c in (chunks - 2, chunks - 1) for k in (1, 0)]


def kernel(
    l_ref, b_ref, x_ref, rb_ref, lg_ref,
    l3_v, b_v, strip_v, x3_v, xo_v, p3_v, p2_v, e0_v,
    b0_rx, b1_rx, b3_rx, l_rx, l3_rx, cross_rx, x3_rx,
    b_tx, fwd_tx, l_tx, l3_tx, x3_tx,
    load_sem, strip_sem, out_sem, l3_sem, piece_sem,
):
    n, m = b_ref.shape
    half = n // 2
    rt = n // TILES
    w = CHUNK
    chunks = m // w
    edge, hw = chunks - 1, w // 2
    batch, row, col = (lax.axis_index(a) for a in ("batch", "row", "col"))
    core_peer = col + 1 - 2 * lax.rem(col, 2)
    y_peer = lax.rem(col + 2, 4)
    far = lax.rem(core_peer + 2, 4)

    def remote(src, dst, send, recv, r, c):
        return pltpu.make_async_remote_copy(
            src_ref=src, dst_ref=dst, send_sem=send, recv_sem=recv,
            device_id=(batch, r, c), device_id_type=MESH,
        )

    def arrived(dst, sem):
        pltpu.make_async_copy(dst, dst, sem).wait()

    def own_chunk(c):
        return b_ref.at[:, pl.ds(pl.multiple_of(c * w, w), w)]

    def x_tile(i, c):
        return x_ref.at[pl.ds(pl.multiple_of(i * rt, rt), rt), pl.ds(pl.multiple_of(c * w, w), w)]

    barrier = pltpu.get_barrier_semaphore()
    greet = functools.partial(pl.semaphore_signal, barrier, inc=1, device_id_type=MESH)
    greet(device_id=(batch, row, core_peer))
    greet(device_id=(batch, row, y_peer))

    @pl.when(row > 0)
    def _():
        greet(device_id=(batch, row - 1, col))

    @pl.when(row < 3)
    def _():
        greet(device_id=(batch, row + 1, col))

    pl.semaphore_wait(barrier, 4 - (row == 0).astype(jnp.int32) - (row == 3).astype(jnp.int32))

    def l_exchange_start():
        remote(l_ref, lg_ref.at[0, col], l_tx.at[0], l_rx.at[0], row, y_peer).start()
        remote(l_ref, lg_ref.at[0, col], l_tx.at[1], l_rx.at[1], row, core_peer).start()

    def l_forward():
        blk = lg_ref.at[0, y_peer]
        arrived(blk, l_rx.at[0])
        remote(blk, blk, l_tx.at[2], l_rx.at[2], row, core_peer).start()

    def l_exchange_end():
        arrived(lg_ref.at[0, core_peer], l_rx.at[1])
        arrived(lg_ref.at[0, far], l_rx.at[2])

    def l_exchange_drain():
        for s in range(3):
            arrived(l_ref, l_tx.at[s])

    def strip_start(r, i):
        slot = lax.rem(i, 2)
        rows = pl.ds(pl.multiple_of(i * rt, rt), rt)
        for k in range(r + 1):
            dst = strip_v.at[slot, :, pl.ds(k * n, n)]

            @pl.when(col == k)
            def _(dst=dst):
                pltpu.make_async_copy(l_ref.at[rows], dst, strip_sem.at[slot]).start()

            @pl.when(col != k)
            def _(dst=dst, k=k):
                pltpu.make_async_copy(lg_ref.at[0, k, rows], dst, strip_sem.at[slot]).start()

    def strip_wait(r, i):
        slot = lax.rem(i, 2)
        ref = strip_v.at[slot, :, pl.ds(0, (r + 1) * n)]
        pltpu.make_async_copy(ref, ref, strip_sem.at[slot]).wait()

    def load(c, slot, k, src):
        return pltpu.make_async_copy(src, b_v.at[slot, pl.ds(k * n, n), :], load_sem.at[slot, k])

    def own_rows(r, c, slot, end):
        depth = (r + 1) * n

        def tile(i, carry):
            part = lax.rem(i, 2)
            strip_wait(r, i)

            @pl.when((i + 1 < TILES) | (c + 1 < end))
            def _():
                strip_start(r, lax.rem(i + 1, TILES))

            out = pltpu.make_async_copy(xo_v.at[part], x_tile(i, c), out_sem.at[part])

            @pl.when((i >= 2) | (c > 0))
            def _():
                out.wait()

            xo_v[part] = jnp.dot(
                strip_v[part, :, :depth], b_v[slot, :depth, :], preferred_element_type=jnp.float32
            ).astype(xo_v.dtype)
            out.start()
            return carry

        lax.fori_loop(0, TILES, tile, 0)

    def own_rows_drain():
        for s in range(2):
            pltpu.make_async_copy(xo_v.at[s], x_tile(s, 0), out_sem.at[s]).wait()

    def simple_rows(r, prior):
        def loads(c, slot):
            return [load(c, slot, k, ref(c)) for k, ref in prior]

        for cp in loads(0, 0):
            cp.start()
        strip_start(r, 0)

        def step(c, carry):
            slot = lax.rem(c, 2)
            for cp in loads(c, slot):
                cp.wait()

            @pl.when(c + 1 < chunks)
            def _():
                for cp in loads(c + 1, 1 - slot):
                    cp.start()

            own_rows(r, c, slot, chunks)
            return carry

        lax.fori_loop(0, chunks, step, 0)
        own_rows_drain()

    @pl.when(row == 0)
    def _():
        def send(c, carry):
            remote(own_chunk(c), rb_ref.at[0, c], b_tx, b0_rx.at[c], 1, col).start()
            return carry

        lax.fori_loop(0, chunks, send, 0)
        l_exchange_start()
        l_forward()
        l_exchange_end()
        simple_rows(0, [(0, own_chunk)])
        l_exchange_drain()
        arrived(b_ref, b_tx)

    @pl.when(row == 1)
    def _():
        l_exchange_start()

        for k, c in mid_order(chunks):
            blk = rb_ref.at[k, c]
            if k == 1:
                remote(own_chunk(c), blk, b_tx, b1_rx.at[c], 2, col).start()
                continue
            arrived(blk, b0_rx.at[c])
            if c < edge:
                remote(blk, blk, fwd_tx, b0_rx.at[c], 2, col).start()
                continue
            for h in range(2):
                half_cols = pl.ds(h * hw, hw)
                remote(blk.at[:, half_cols], e0_v.at[:, half_cols], fwd_tx, b0_rx.at[c + h], 2, col).start()
        l_forward()
        l_exchange_end()
        simple_rows(1, [(0, lambda c: rb_ref.at[0, c]), (1, own_chunk)])
        l_exchange_drain()
        arrived(b_ref, b_tx)
        arrived(rb_ref.at[0], fwd_tx)

    @pl.when(row == 2)
    def _():
        l_exchange_start()
        lo, hi = pl.ds(0, half), pl.ds(half, half)

        def own(p):
            return lg_ref.at[1, col, p]

        def other(p):
            return lg_ref.at[1, y_peer, p]

        arrived(own(lo), l3_rx.at[0])
        remote(own(lo), own(lo), l3_tx.at[0], l3_rx.at[2], row, y_peer).start()
        remote(own(lo), own(lo), l3_tx.at[1], l3_rx.at[4], row, core_peer).start()
        arrived(own(hi), l3_rx.at[1])
        remote(own(hi), own(hi), l3_tx.at[2], l3_rx.at[5], row, core_peer).start()
        l_forward()
        arrived(other(lo), l3_rx.at[2])
        remote(other(lo), other(lo), l3_tx.at[3], l3_rx.at[6], row, core_peer).start()
        arrived(other(hi), l3_rx.at[3])
        remote(other(hi), other(hi), l3_tx.at[4], l3_rx.at[7], row, core_peer).start()
        l_exchange_end()
        for s, (blk, p) in enumerate(((core_peer, lo), (core_peer, hi), (far, lo), (far, hi))):
            arrived(lg_ref.at[1, blk, p], l3_rx.at[4 + s])
        for k in range(4):
            pltpu.make_async_copy(lg_ref.at[1, k], l3_v.at[:, pl.ds(k * n, n)], l3_sem).start()

        def load1(c, slot):
            return load(c, slot, 1, rb_ref.at[1, c])

        def load23(c, slot):
            return load(c, slot, 2, own_chunk(c)), load(c, slot, 3, rb_ref.at[2, c])

        def prefetch23(c, slot):
            arrived(rb_ref.at[2, c], b3_rx.at[c])
            for cp in load23(c, slot):
                cp.start()

        def prefetch1(c, slot):
            arrived(rb_ref.at[1, c], b1_rx.at[c])
            load1(c, slot).start()

        def x3_send(i, c, slot):
            return remote(x3_v.at[slot, i], x_tile(i, c), x3_tx.at[slot, i], x3_rx, 3, col)

        prefetch23(0, 0)
        prefetch1(0, 0)
        strip_start(2, 0)
        pltpu.make_async_copy(l3_v, l3_v, l3_sem).wait()

        e_slot, e_spare = edge % 2, 1 - edge % 2

        def piece(s):
            q = lax.rem(s, 6)
            return strip_v.at[q // 3, :, pl.ds(pl.multiple_of(lax.rem(q, 3) * n, n), n)]

        def piece_start(s):
            k, i = 2 - s // TILES, s % TILES
            rows = pl.ds(i * rt, rt)

            @pl.when(col == k)
            def _():
                pltpu.make_async_copy(l_ref.at[rows], piece(s), piece_sem.at[s]).start()

            @pl.when(col != k)
            def _():
                pltpu.make_async_copy(lg_ref.at[0, k, rows], piece(s), piece_sem.at[s]).start()

        def piece_wait(s):
            arrived(piece(s), piece_sem.at[s])

        def tile_rows(i):
            return pl.ds(pl.multiple_of(i * rt, rt), rt)

        def dot(a, b):
            return jnp.dot(a, b, preferred_element_type=jnp.float32)

        def terms23():
            for s in range(TILES):
                piece_start(s)
            prefetch23(edge, e_slot)
            for cp in load23(edge, e_slot):
                cp.wait()

            def tile(i, carry):
                rows = tile_rows(i)
                p3_v[rows, :] = dot(l3_v[rows, 2 * n :], b_v[e_slot, 2 * n :, :])
                piece_wait(i)
                p2_v[rows, :] = dot(piece(i)[...], b_v[e_slot, 2 * n : 3 * n, :])
                return carry

            lax.fori_loop(0, TILES, tile, 0)
            prefetch1(edge - 1, e_spare)
            strip_start(2, 0)

        def step(c, carry):
            slot = lax.rem(c, 2)
            pl.when(c == edge - 1)(terms23)
            arrived(rb_ref.at[0, c], b0_rx.at[c])
            last = load(c, slot, 0, rb_ref.at[0, c])
            last.start()
            for cp in (load1(c, slot), *load23(c, slot), last):
                cp.wait()
            def tile(i, inner):
                @pl.when(c >= 2)
                def _():
                    x3_send(i, c, slot).wait_send()

                rows = pl.ds(pl.multiple_of(i * rt, rt), rt)
                x3_v[slot, i] = jnp.dot(
                    l3_v[rows, :], b_v[slot], preferred_element_type=jnp.float32
                ).astype(x3_v.dtype)

                @pl.when(i > 0)
                def _():
                    x3_send(i - 1, c, slot).start()

                return inner

            lax.fori_loop(0, TILES, tile, 0)

            x3_send(TILES - 1, c, slot).start()

            @pl.when(c + 1 < edge)
            def _():
                prefetch23(c + 1, 1 - slot)

            @pl.when(c + 2 < edge)
            def _():
                prefetch1(c + 1, 1 - slot)

            own_rows(2, c, slot, edge - 1)
            return carry

        lax.fori_loop(0, edge, step, 0)
        own_rows_drain()

        for s in range(TILES, TILES + 6):
            piece_start(s)
        prefetch1(edge, e_slot)
        load1(edge, e_slot).wait()

        def terms1_x3(i, carry):
            rows = tile_rows(i)
            p3_v[rows, :] += dot(l3_v[rows, n : 2 * n], b_v[e_slot, n : 2 * n, :])
            return carry

        def terms1_x2(i, carry):
            piece_wait(TILES + i)
            p2_v[tile_rows(i), :] += dot(piece(TILES + i)[...], b_v[e_slot, n : 2 * n, :])
            return carry

        lax.fori_loop(0, TILES, terms1_x3, 0)
        for s in range(2):
            for i in range(TILES):
                x3_send(i, 0, s).wait_send()

        def half_lanes(h):
            return pl.ds(pl.multiple_of(h * hw, hw), hw)

        def x3_half(i, h):
            lanes = pl.ds(pl.multiple_of(edge * w + h * hw, hw), hw)
            return remote(
                x3_v.at[e_slot, i, :, half_lanes(h)], x_ref.at[tile_rows(i), lanes], x3_tx.at[e_slot, i], x3_rx, 3, col
            )

        def half_step(h, carry):
            lanes = half_lanes(h)
            arrived(e0_v.at[:, lanes], b0_rx.at[edge + h])

            def tile(i, inner):
                rows = tile_rows(i)
                x3_v[e_slot, i, :, lanes] = (
                    p3_v[rows, lanes] + dot(l3_v[rows, :n], e0_v[:, lanes])
                ).astype(x3_v.dtype)

                @pl.when(i > 0)
                def _():
                    x3_half(i - 1, h).start()

                return inner

            lax.fori_loop(0, TILES, tile, 0)

            @pl.when(h == 0)
            def _():
                lax.fori_loop(0, TILES, terms1_x2, 0)
                for s in range(TILES + 6, 3 * TILES):
                    piece_start(s)

            x3_half(TILES - 1, h).start()
            return carry

        lax.fori_loop(0, 2, half_step, 0)

        def x2_edge(i):
            return pltpu.make_async_copy(x3_v.at[e_spare, i], x_tile(i, edge), x3_tx.at[e_spare, i])

        def terms0_x2(i, carry):
            piece_wait(2 * TILES + i)
            x3_v[e_spare, i] = (
                p2_v[tile_rows(i), :] + dot(piece(2 * TILES + i)[...], e0_v[...])
            ).astype(x3_v.dtype)

            @pl.when(i > 0)
            def _():
                x2_edge(i - 1).start()

            return carry

        lax.fori_loop(0, TILES, terms0_x2, 0)
        x2_edge(TILES - 1).start()
        for s in range(2):
            for i in range(TILES):
                arrived(x3_v.at[s, i], x3_tx.at[s, i])
        l_exchange_drain()
        for s in range(5):
            arrived(own(lo), l3_tx.at[s])

    @pl.when(row == 3)
    def _():
        lo, hi = pl.ds(0, half), pl.ds(half, half)
        for s, p in enumerate((lo, hi)):
            remote(l_ref.at[p], lg_ref.at[1, col, p], l3_tx.at[s], l3_rx.at[s], 2, col).start()
        remote(l_ref.at[hi], lg_ref.at[1, col, hi], l3_tx.at[2], cross_rx, row, y_peer).start()
        blk = lg_ref.at[1, y_peer, hi]
        arrived(blk, cross_rx)
        remote(blk, blk, l3_tx.at[3], l3_rx.at[3], 2, col).start()

        def send(c, carry):
            remote(own_chunk(c), rb_ref.at[2, c], b_tx, b3_rx.at[c], 2, col).start()
            return carry

        lax.fori_loop(0, chunks, send, 0)
        for s in range(4):
            arrived(blk, l3_tx.at[s])
        arrived(b_ref, b_tx)
        arrived(x_ref, x3_rx)


def copy_kernel(src_ref, dst_ref, buf, in_sem, out_sem):
    parts, rows, _ = buf.shape

    def fetch(s):
        return pltpu.make_async_copy(src_ref.at[pl.ds(s * rows, rows)], buf.at[s], in_sem.at[s])

    def store(s):
        return pltpu.make_async_copy(buf.at[s], dst_ref.at[pl.ds(s * rows, rows)], out_sem.at[s])

    for s in range(parts):
        fetch(s).start()
    for s in range(parts):
        fetch(s).wait()
        store(s).start()
    for s in range(parts):
        store(s).wait()


def solution(mesh):
    block_spec = P(("batch", "row"), "col")

    def local_product(l_block, b_block):
        n, m = b_block.shape
        rt = n // TILES
        chunks = m // CHUNK
        dma = pltpu.SemaphoreType.DMA
        hbm = pl.BlockSpec(memory_space=pl.ANY)
        x, _, _ = pl.pallas_call(
            kernel,
            out_shape=(
                jax.ShapeDtypeStruct((n, m), b_block.dtype),
                jax.ShapeDtypeStruct((3, chunks, n, CHUNK), b_block.dtype),
                jax.ShapeDtypeStruct((2, 4, n, n), l_block.dtype),
            ),
            in_specs=[hbm, hbm],
            out_specs=(hbm, hbm, hbm),
            scratch_shapes=[
                pltpu.VMEM((n, 4 * n), l_block.dtype),
                pltpu.VMEM((2, 4 * n, CHUNK), b_block.dtype),
                pltpu.VMEM((2, rt, 3 * n), l_block.dtype),
                pltpu.VMEM((2, TILES, rt, CHUNK), b_block.dtype),
                pltpu.VMEM((2, rt, CHUNK), b_block.dtype),
                pltpu.VMEM((n, CHUNK), jnp.float32),
                pltpu.VMEM((n, CHUNK), jnp.float32),
                pltpu.VMEM((n, CHUNK), b_block.dtype),
                dma((chunks + 1,)), dma((chunks,)), dma((chunks,)), dma((3,)), dma((8,)), dma, dma,
                dma, dma, dma((3,)), dma((5,)), dma((2, TILES)),
                dma((2, 4)), dma((2,)), dma((2,)), dma, dma((12,)),
            ],
            compiler_params=pltpu.CompilerParams(has_side_effects=True, collective_id=0, vmem_limit_bytes=66 * 1000 * 1000),
        )(l_block, b_block)
        return pl.pallas_call(
            copy_kernel,
            out_shape=jax.ShapeDtypeStruct((n, m), x.dtype),
            in_specs=[hbm],
            out_specs=hbm,
            scratch_shapes=[pltpu.VMEM((PARTS, n // PARTS, m), x.dtype), dma((PARTS,)), dma((PARTS,))],
            compiler_params=pltpu.CompilerParams(vmem_limit_bytes=66 * 1000 * 1000),
        )(x)

    return jax.shard_map(
        local_product, mesh=mesh, in_specs=(block_spec, block_spec), out_specs=block_spec, check_vma=False
    )
```

```python
import functools

import jax
import jax.numpy as jnp
from jax import lax
from jax.experimental import pallas as pl
from jax.experimental.pallas import tpu as pltpu
from jax.sharding import PartitionSpec as P

MESH = pl.DeviceIdType.MESH
PARTS = 8
TILES = 4
CHUNK = 256
LAST = 2


def mid_order(lead):
    first = lead - 2
    late = list(range(first, lead))
    gap = -(-lead // 3)
    order = [(1, c) for c in range(first)]
    for c in range(lead):
        order.append((0, c))
        if late and (c + 1) % gap == 0:
            order.append((1, late.pop(0)))
    assert not late
    return order


def kernel(
    l_ref, b_ref, x_ref, rb_ref, lg_ref,
    l3_v, b_v, strip_v, x3_v, xo_v, xs_v,
    b0_rx, b1_rx, b3_rx, l_rx, l2_rx, l3_rx, cross_rx, x3_rx, xs_rx,
    b_tx, fwd_tx, l_tx, l2_tx, l3_tx, x3_tx, xs_tx,
    load_sem, strip_sem, out_sem, l3_sem,
):
    n, m = b_ref.shape
    half = n // 2
    rt = n // TILES
    w = CHUNK
    chunks = m // w
    lead = chunks - LAST
    batch, row, col = (lax.axis_index(a) for a in ("batch", "row", "col"))
    core_peer = col + 1 - 2 * lax.rem(col, 2)
    y_peer = lax.rem(col + 2, 4)
    far = lax.rem(core_peer + 2, 4)

    def remote(src, dst, send, recv, r, c):
        return pltpu.make_async_remote_copy(
            src_ref=src, dst_ref=dst, send_sem=send, recv_sem=recv,
            device_id=(batch, r, c), device_id_type=MESH,
        )

    def arrived(dst, sem):
        pltpu.make_async_copy(dst, dst, sem).wait()

    def lead_part(ref):
        return ref.at[:, pl.ds(0, lead * w)]

    def last_part(ref):
        return ref.at[:, pl.ds(lead * w, LAST * w)]

    def dot(a, b):
        return jnp.dot(a, b, preferred_element_type=jnp.float32)

    def tile_rows(i):
        return pl.ds(pl.multiple_of(i * rt, rt), rt)

    def l3_load():
        for k in range(4):
            pltpu.make_async_copy(lg_ref.at[1, k], l3_v.at[:, pl.ds(k * n, n)], l3_sem).start()

    def own_chunk(c):
        return b_ref.at[:, pl.ds(pl.multiple_of(c * w, w), w)]

    def x_tile(i, c):
        return x_ref.at[pl.ds(pl.multiple_of(i * rt, rt), rt), pl.ds(pl.multiple_of(c * w, w), w)]

    barrier = pltpu.get_barrier_semaphore()
    greet = functools.partial(pl.semaphore_signal, barrier, inc=1, device_id_type=MESH)
    greet(device_id=(batch, row, core_peer))
    greet(device_id=(batch, row, y_peer))

    @pl.when(row > 0)
    def _():
        greet(device_id=(batch, row - 1, col))

    @pl.when(row < 3)
    def _():
        greet(device_id=(batch, row + 1, col))

    @pl.when((row == 1) | (row == 3))
    def _():
        greet(device_id=(batch, 4 - row, col))

    pl.semaphore_wait(barrier, 3 + jnp.where(row == 0, 0, jnp.where(row == 1, 2, 1)))

    def l_exchange_start():
        remote(l_ref, lg_ref.at[0, col], l_tx.at[0], l_rx.at[0], row, y_peer).start()
        remote(l_ref, lg_ref.at[0, col], l_tx.at[1], l_rx.at[1], row, core_peer).start()

    def l_forward():
        blk = lg_ref.at[0, y_peer]
        arrived(blk, l_rx.at[0])
        remote(blk, blk, l_tx.at[2], l_rx.at[2], row, core_peer).start()

    def l_exchange_end():
        arrived(lg_ref.at[0, core_peer], l_rx.at[1])
        arrived(lg_ref.at[0, far], l_rx.at[2])

    def l_exchange_drain():
        for s in range(3):
            arrived(l_ref, l_tx.at[s])

    def strip_start(r, i):
        slot = lax.rem(i, 2)
        rows = pl.ds(pl.multiple_of(i * rt, rt), rt)
        for k in range(r + 1):
            dst = strip_v.at[slot, :, pl.ds(k * n, n)]

            @pl.when(col == k)
            def _(dst=dst):
                pltpu.make_async_copy(l_ref.at[rows], dst, strip_sem.at[slot]).start()

            @pl.when(col != k)
            def _(dst=dst, k=k):
                pltpu.make_async_copy(lg_ref.at[0, k, rows], dst, strip_sem.at[slot]).start()

    def strip_wait(r, i):
        slot = lax.rem(i, 2)
        ref = strip_v.at[slot, :, pl.ds(0, (r + 1) * n)]
        pltpu.make_async_copy(ref, ref, strip_sem.at[slot]).wait()

    def load(c, slot, k, src):
        return pltpu.make_async_copy(src, b_v.at[slot, pl.ds(k * n, n), :], load_sem.at[slot, k])

    def own_rows(r, c, slot, end):
        depth = (r + 1) * n

        def tile(i, carry):
            part = lax.rem(i, 2)
            strip_wait(r, i)

            @pl.when((i + 1 < TILES) | (c + 1 < end))
            def _():
                strip_start(r, lax.rem(i + 1, TILES))

            out = pltpu.make_async_copy(xo_v.at[part], x_tile(i, c), out_sem.at[part])

            @pl.when((i >= 2) | (c > 0))
            def _():
                out.wait()

            xo_v[part] = jnp.dot(
                strip_v[part, :, :depth], b_v[slot, :depth, :], preferred_element_type=jnp.float32
            ).astype(xo_v.dtype)
            out.start()
            return carry

        lax.fori_loop(0, TILES, tile, 0)

    def own_rows_drain():
        for s in range(2):
            pltpu.make_async_copy(xo_v.at[s], x_tile(s, 0), out_sem.at[s]).wait()

    def simple_rows(r, prior):
        def loads(c, slot):
            return [load(c, slot, k, ref(c)) for k, ref in prior]

        for cp in loads(0, 0):
            cp.start()
        strip_start(r, 0)

        def step(c, carry):
            slot = lax.rem(c, 2)
            for cp in loads(c, slot):
                cp.wait()

            @pl.when(c + 1 < chunks)
            def _():
                for cp in loads(c + 1, 1 - slot):
                    cp.start()

            own_rows(r, c, slot, chunks)
            return carry

        lax.fori_loop(0, chunks, step, 0)
        own_rows_drain()

    @pl.when(row == 0)
    def _():
        def send(c, carry):
            remote(own_chunk(c), rb_ref.at[0, c], b_tx, b0_rx.at[c], 1, col).start()
            return carry

        lax.fori_loop(0, chunks, send, 0)
        l_exchange_start()
        l_forward()
        l_exchange_end()
        simple_rows(0, [(0, own_chunk)])
        l_exchange_drain()
        arrived(b_ref, b_tx)

    @pl.when(row == 1)
    def _():
        l_exchange_start()

        def share(q, rx, tx):
            own = lg_ref.at[q, col]
            remote(own, own, tx.at[0], rx.at[1], row, y_peer).start()
            remote(own, own, tx.at[1], rx.at[2], row, core_peer).start()

        def share_forward(q, rx, tx):
            blk = lg_ref.at[q, y_peer]
            arrived(blk, rx.at[1])
            remote(blk, blk, tx.at[2], rx.at[3], row, core_peer).start()

        def share_end(q, rx):
            arrived(lg_ref.at[q, core_peer], rx.at[2])
            arrived(lg_ref.at[q, far], rx.at[3])

        def b0_arrived(c):
            arrived(rb_ref.at[0, c], b0_rx.at[c])

        for k, c in mid_order(lead):
            blk = rb_ref.at[k, c]
            if k == 1:
                remote(own_chunk(c), blk, b_tx, b1_rx.at[c], 2, col).start()
                continue
            b0_arrived(c)
            remote(blk, blk, fwd_tx, b0_rx.at[c], 2, col).start()
            if c == chunks // 2:
                l_forward()
                arrived(lg_ref.at[2, col], l2_rx.at[0])
                share(2, l2_rx, l2_tx)
        for c in range(lead, chunks):
            b0_arrived(c)
        arrived(lg_ref.at[1, col], l3_rx.at[0])
        share(1, l3_rx, l3_tx)
        share_forward(2, l2_rx, l2_tx)
        share_end(2, l2_rx)

        def last_loads(blocks):
            return [load(lead + j, j, k, ref(lead + j)) for j in range(LAST) for k, ref in blocks]

        b012 = [(0, lambda c: rb_ref.at[0, c]), (1, own_chunk), (2, lambda c: rb_ref.at[1, c])]
        b3 = [(3, lambda c: rb_ref.at[2, c])]

        def send_last(q, r):
            def one(t, carry):
                i, j = t // LAST, lax.rem(t, LAST)
                remote(xs_v.at[q, j, i], x_tile(i, lead + j), xs_tx.at[q], xs_rx.at[q], r, col).start()
                return carry

            lax.fori_loop(0, TILES * LAST, one, 0)

        for c in range(lead, chunks):
            arrived(rb_ref.at[1, c], b1_rx.at[c])
        for cp in last_loads(b012):
            cp.start()

        def last_strip(i):
            part = lax.rem(i, 2)
            return [
                pltpu.make_async_copy(
                    lg_ref.at[2, k, tile_rows(i)], strip_v.at[part, :, pl.ds(k * n, n)], strip_sem.at[part]
                )
                for k in range(3)
            ]

        for cp in last_strip(0):
            cp.start()
        for cp in last_loads(b012):
            cp.wait()

        def tile2(i, carry):
            for cp in last_strip(i):
                cp.wait()

            @pl.when(i + 1 < TILES)
            def _():
                for cp in last_strip(i + 1):
                    cp.start()

            for j in range(LAST):
                xs_v[0, j, i] = dot(strip_v[lax.rem(i, 2)], b_v[j, : 3 * n, :]).astype(xs_v.dtype)
            return carry

        lax.fori_loop(0, TILES, tile2, 0)
        send_last(0, 2)

        l_exchange_end()
        simple_rows(1, [(0, lambda c: rb_ref.at[0, c]), (1, own_chunk)])

        share_forward(1, l3_rx, l3_tx)
        share_end(1, l3_rx)
        l3_load()
        for c in range(lead, chunks):
            arrived(rb_ref.at[2, c], b3_rx.at[c])
        for cp in last_loads(b012 + b3):
            cp.start()
        for cp in last_loads(b012 + b3):
            cp.wait()
        arrived(l3_v, l3_sem)

        def tile3(i, carry):
            for j in range(LAST):
                xs_v[1, j, i] = dot(l3_v[tile_rows(i), :], b_v[j]).astype(xs_v.dtype)
            return carry

        lax.fori_loop(0, TILES, tile3, 0)
        send_last(1, 3)

        l_exchange_drain()
        for s in range(3):
            arrived(l_ref, l2_tx.at[s])
            arrived(l_ref, l3_tx.at[s])
        arrived(lead_part(b_ref), b_tx)
        arrived(lead_part(b_ref), fwd_tx)
        for q in range(2):
            arrived(xs_v.at[q], xs_tx.at[q])

    @pl.when(row == 2)
    def _():
        l_exchange_start()
        lo, hi = pl.ds(0, half), pl.ds(half, half)

        def own(p):
            return lg_ref.at[1, col, p]

        def other(p):
            return lg_ref.at[1, y_peer, p]

        remote(l_ref, lg_ref.at[2, col], l2_tx.at[0], l2_rx.at[0], 1, col).start()
        for c in range(lead, chunks):
            remote(own_chunk(c), rb_ref.at[1, c], b_tx, b1_rx.at[c], 1, col).start()

        arrived(own(lo), l3_rx.at[0])
        remote(own(lo), own(lo), l3_tx.at[0], l3_rx.at[2], row, y_peer).start()
        remote(own(lo), own(lo), l3_tx.at[1], l3_rx.at[4], row, core_peer).start()
        arrived(own(hi), l3_rx.at[1])
        remote(lg_ref.at[1, col], lg_ref.at[1, col], l2_tx.at[1], l3_rx.at[0], 1, col).start()
        remote(own(hi), own(hi), l3_tx.at[2], l3_rx.at[5], row, core_peer).start()
        l_forward()
        arrived(other(lo), l3_rx.at[2])
        remote(other(lo), other(lo), l3_tx.at[3], l3_rx.at[6], row, core_peer).start()
        arrived(other(hi), l3_rx.at[3])
        remote(other(hi), other(hi), l3_tx.at[4], l3_rx.at[7], row, core_peer).start()
        l_exchange_end()
        for s, (blk, p) in enumerate(((core_peer, lo), (core_peer, hi), (far, lo), (far, hi))):
            arrived(lg_ref.at[1, blk, p], l3_rx.at[4 + s])
        l3_load()

        def early(c, slot):
            return (
                load(c, slot, 1, rb_ref.at[1, c]), load(c, slot, 2, own_chunk(c)), load(c, slot, 3, rb_ref.at[2, c])
            )

        def prefetch(c, slot):
            arrived(rb_ref.at[1, c], b1_rx.at[c])
            arrived(rb_ref.at[2, c], b3_rx.at[c])
            for cp in early(c, slot):
                cp.start()

        def x3_send(i, c, slot):
            return remote(x3_v.at[slot, i], x_tile(i, c), x3_tx.at[slot, i], x3_rx, 3, col)

        prefetch(0, 0)
        strip_start(2, 0)
        pltpu.make_async_copy(l3_v, l3_v, l3_sem).wait()

        def step(c, carry):
            slot = lax.rem(c, 2)
            arrived(rb_ref.at[0, c], b0_rx.at[c])
            last = load(c, slot, 0, rb_ref.at[0, c])
            last.start()
            for cp in (*early(c, slot), last):
                cp.wait()
            def tile(i, inner):
                @pl.when(c >= 2)
                def _():
                    x3_send(i, c, slot).wait_send()

                rows = pl.ds(pl.multiple_of(i * rt, rt), rt)
                x3_v[slot, i] = jnp.dot(
                    l3_v[rows, :], b_v[slot], preferred_element_type=jnp.float32
                ).astype(x3_v.dtype)

                @pl.when(i > 0)
                def _():
                    x3_send(i - 1, c, slot).start()

                return inner

            lax.fori_loop(0, TILES, tile, 0)

            x3_send(TILES - 1, c, slot).start()

            @pl.when(c + 1 < lead)
            def _():
                prefetch(c + 1, 1 - slot)

            own_rows(2, c, slot, lead)
            return carry

        lax.fori_loop(0, lead, step, 0)
        own_rows_drain()
        for s in range(2):
            for i in range(TILES):
                x3_send(i, 0, s).wait_send()
        arrived(last_part(x_ref), xs_rx.at[0])
        for s in range(2):
            arrived(l_ref, l2_tx.at[s])
        arrived(last_part(b_ref), b_tx)
        l_exchange_drain()
        for s in range(5):
            arrived(own(lo), l3_tx.at[s])

    @pl.when(row == 3)
    def _():
        lo, hi = pl.ds(0, half), pl.ds(half, half)
        for s, p in enumerate((lo, hi)):
            remote(l_ref.at[p], lg_ref.at[1, col, p], l3_tx.at[s], l3_rx.at[s], 2, col).start()
        remote(l_ref.at[hi], lg_ref.at[1, col, hi], l3_tx.at[2], cross_rx, row, y_peer).start()
        blk = lg_ref.at[1, y_peer, hi]
        arrived(blk, cross_rx)
        remote(blk, blk, l3_tx.at[3], l3_rx.at[3], 2, col).start()

        def send(first, end, r):
            def one(c, carry):
                remote(own_chunk(c), rb_ref.at[2, c], b_tx, b3_rx.at[c], r, col).start()
                return carry

            lax.fori_loop(first, end, one, 0)

        mark = lead * 5 // 7
        send(0, mark, 2)
        send(lead, chunks, 1)
        send(mark, lead, 2)
        for s in range(4):
            arrived(blk, l3_tx.at[s])
        arrived(b_ref, b_tx)
        arrived(lead_part(x_ref), x3_rx)
        arrived(last_part(x_ref), xs_rx.at[1])


def copy_kernel(src_ref, dst_ref, buf, in_sem, out_sem):
    parts, rows, _ = buf.shape

    def fetch(s):
        return pltpu.make_async_copy(src_ref.at[pl.ds(s * rows, rows)], buf.at[s], in_sem.at[s])

    def store(s):
        return pltpu.make_async_copy(buf.at[s], dst_ref.at[pl.ds(s * rows, rows)], out_sem.at[s])

    for s in range(parts):
        fetch(s).start()
    for s in range(parts):
        fetch(s).wait()
        store(s).start()
    for s in range(parts):
        store(s).wait()


def solution(mesh):
    block_spec = P(("batch", "row"), "col")

    def local_product(l_block, b_block):
        n, m = b_block.shape
        rt = n // TILES
        chunks = m // CHUNK
        dma = pltpu.SemaphoreType.DMA
        hbm = pl.BlockSpec(memory_space=pl.ANY)
        x, _, _ = pl.pallas_call(
            kernel,
            out_shape=(
                jax.ShapeDtypeStruct((n, m), b_block.dtype),
                jax.ShapeDtypeStruct((3, chunks, n, CHUNK), b_block.dtype),
                jax.ShapeDtypeStruct((3, 4, n, n), l_block.dtype),
            ),
            in_specs=[hbm, hbm],
            out_specs=(hbm, hbm, hbm),
            scratch_shapes=[
                pltpu.VMEM((n, 4 * n), l_block.dtype),
                pltpu.VMEM((2, 4 * n, CHUNK), b_block.dtype),
                pltpu.VMEM((2, rt, 3 * n), l_block.dtype),
                pltpu.VMEM((2, TILES, rt, CHUNK), b_block.dtype),
                pltpu.VMEM((2, rt, CHUNK), b_block.dtype),
                pltpu.VMEM((2, LAST, TILES, rt, CHUNK), b_block.dtype),
                dma((chunks,)), dma((chunks,)), dma((chunks,)), dma((3,)), dma((4,)), dma((8,)), dma, dma, dma((2,)),
                dma, dma, dma((3,)), dma((3,)), dma((5,)), dma((2, TILES)), dma((2,)),
                dma((2, 4)), dma((2,)), dma((2,)), dma,
            ],
            compiler_params=pltpu.CompilerParams(has_side_effects=True, collective_id=0, vmem_limit_bytes=66 * 1000 * 1000),
        )(l_block, b_block)
        return pl.pallas_call(
            copy_kernel,
            out_shape=jax.ShapeDtypeStruct((n, m), x.dtype),
            in_specs=[hbm],
            out_specs=hbm,
            scratch_shapes=[pltpu.VMEM((PARTS, n // PARTS, m), x.dtype), dma((PARTS,)), dma((PARTS,))],
            compiler_params=pltpu.CompilerParams(vmem_limit_bytes=66 * 1000 * 1000),
        )(x)

    return jax.shard_map(
        local_product, mesh=mesh, in_specs=(block_spec, block_spec), out_specs=block_spec, check_vma=False
    )
```

```python
import functools

import jax
import jax.numpy as jnp
from jax import lax
from jax.experimental import pallas as pl
from jax.experimental.pallas import tpu as pltpu
from jax.sharding import PartitionSpec as P

MESH = pl.DeviceIdType.MESH
PARTS = 8
TILES = 4
CHUNK = 256
TAIL = 256
LAST = 2


def mid_order(lead):
    first = lead - 2
    late = list(range(first, lead))
    gap = -(-lead // 3)
    order = [(1, c) for c in range(first)]
    for c in range(lead):
        order.append((0, c))
        if late and (c + 1) % gap == 0:
            order.append((1, late.pop(0)))
    assert not late
    return order


def kernel(
    l_ref, b_ref, x_ref, rb_ref, lg_ref, t_ref,
    l3_v, b_v, strip_v, x3_v, xo_v, xs_v,
    b0_rx, b1_rx, b3_rx, l_rx, l2_rx, l3_rx, cross_rx, x3_rx, xs_rx,
    b_tx, fwd_tx, l_tx, l2_tx, l3_tx, x3_tx, xs_tx,
    load_sem, strip_sem, out_sem, l3_sem,
):
    n, m = b_ref.shape
    half = n // 2
    rt = n // TILES
    w = CHUNK
    chunks = m // w
    lead = chunks - LAST
    batch, row, col = (lax.axis_index(a) for a in ("batch", "row", "col"))
    core_peer = col + 1 - 2 * lax.rem(col, 2)
    y_peer = lax.rem(col + 2, 4)
    far = lax.rem(core_peer + 2, 4)

    def remote(src, dst, send, recv, r, c):
        return pltpu.make_async_remote_copy(
            src_ref=src, dst_ref=dst, send_sem=send, recv_sem=recv,
            device_id=(batch, r, c), device_id_type=MESH,
        )

    def arrived(dst, sem):
        pltpu.make_async_copy(dst, dst, sem).wait()

    def lead_part(ref):
        return ref.at[:, pl.ds(0, lead * w)]

    def last_part(ref):
        return ref.at[:, pl.ds(lead * w, LAST * w)]

    def dot(a, b):
        return jnp.dot(a, b, preferred_element_type=jnp.float32)

    def tile_rows(i):
        return pl.ds(pl.multiple_of(i * rt, rt), rt)

    def l3_load():
        for k in range(4):
            pltpu.make_async_copy(lg_ref.at[1, k], l3_v.at[:, pl.ds(k * n, n)], l3_sem).start()

    def own_chunk(c):
        return b_ref.at[:, pl.ds(pl.multiple_of(c * w, w), w)]

    def x_tile(i, c):
        return x_ref.at[pl.ds(pl.multiple_of(i * rt, rt), rt), pl.ds(pl.multiple_of(c * w, w), w)]

    barrier = pltpu.get_barrier_semaphore()
    greet = functools.partial(pl.semaphore_signal, barrier, inc=1, device_id_type=MESH)
    greet(device_id=(batch, row, core_peer))
    greet(device_id=(batch, row, y_peer))

    @pl.when(row > 0)
    def _():
        greet(device_id=(batch, row - 1, col))

    @pl.when(row < 3)
    def _():
        greet(device_id=(batch, row + 1, col))

    @pl.when((row == 1) | (row == 3))
    def _():
        greet(device_id=(batch, 4 - row, col))

    pl.semaphore_wait(barrier, 3 + jnp.where(row == 0, 0, jnp.where(row == 1, 2, 1)))

    def l_exchange_start():
        remote(l_ref, lg_ref.at[0, col], l_tx.at[0], l_rx.at[0], row, y_peer).start()
        remote(l_ref, lg_ref.at[0, col], l_tx.at[1], l_rx.at[1], row, core_peer).start()

    def l_forward():
        blk = lg_ref.at[0, y_peer]
        arrived(blk, l_rx.at[0])
        remote(blk, blk, l_tx.at[2], l_rx.at[2], row, core_peer).start()

    def l_exchange_end():
        arrived(lg_ref.at[0, core_peer], l_rx.at[1])
        arrived(lg_ref.at[0, far], l_rx.at[2])

    def l_exchange_drain():
        for s in range(3):
            arrived(l_ref, l_tx.at[s])

    def strip_start(r, i):
        slot = lax.rem(i, 2)
        rows = pl.ds(pl.multiple_of(i * rt, rt), rt)
        for k in range(r + 1):
            dst = strip_v.at[slot, :, pl.ds(k * n, n)]

            @pl.when(col == k)
            def _(dst=dst):
                pltpu.make_async_copy(l_ref.at[rows], dst, strip_sem.at[slot]).start()

            @pl.when(col != k)
            def _(dst=dst, k=k):
                pltpu.make_async_copy(lg_ref.at[0, k, rows], dst, strip_sem.at[slot]).start()

    def strip_wait(r, i):
        slot = lax.rem(i, 2)
        ref = strip_v.at[slot, :, pl.ds(0, (r + 1) * n)]
        pltpu.make_async_copy(ref, ref, strip_sem.at[slot]).wait()

    def load(c, slot, k, src):
        return pltpu.make_async_copy(src, b_v.at[slot, pl.ds(k * n, n), :], load_sem.at[slot, k])

    def own_rows(r, c, slot, end):
        depth = (r + 1) * n

        def tile(i, carry):
            part = lax.rem(i, 2)
            strip_wait(r, i)

            @pl.when((i + 1 < TILES) | (c + 1 < end))
            def _():
                strip_start(r, lax.rem(i + 1, TILES))

            out = pltpu.make_async_copy(xo_v.at[part], x_tile(i, c), out_sem.at[part])

            @pl.when((i >= 2) | (c > 0))
            def _():
                out.wait()

            xo_v[part] = jnp.dot(
                strip_v[part, :, :depth], b_v[slot, :depth, :], preferred_element_type=jnp.float32
            ).astype(xo_v.dtype)
            out.start()
            return carry

        lax.fori_loop(0, TILES, tile, 0)

    def own_rows_drain():
        for s in range(2):
            pltpu.make_async_copy(xo_v.at[s], x_tile(s, 0), out_sem.at[s]).wait()

    def simple_rows(r, prior):
        def loads(c, slot):
            return [load(c, slot, k, ref(c)) for k, ref in prior]

        for cp in loads(0, 0):
            cp.start()
        strip_start(r, 0)

        def step(c, carry):
            slot = lax.rem(c, 2)
            for cp in loads(c, slot):
                cp.wait()

            @pl.when(c + 1 < chunks)
            def _():
                for cp in loads(c + 1, 1 - slot):
                    cp.start()

            own_rows(r, c, slot, chunks)
            return carry

        lax.fori_loop(0, chunks, step, 0)
        own_rows_drain()

    @pl.when(row == 0)
    def _():
        def send(c, carry):
            remote(own_chunk(c), rb_ref.at[0, c], b_tx, b0_rx.at[c], 1, col).start()
            return carry

        lax.fori_loop(0, chunks, send, 0)
        l_exchange_start()
        l_forward()
        l_exchange_end()
        simple_rows(0, [(0, own_chunk)])
        l_exchange_drain()
        arrived(b_ref, b_tx)

    @pl.when(row == 1)
    def _():
        l_exchange_start()

        def share(q, rx, tx):
            own = lg_ref.at[q, col]
            remote(own, own, tx.at[0], rx.at[1], row, y_peer).start()
            remote(own, own, tx.at[1], rx.at[2], row, core_peer).start()

        def share_forward(q, rx, tx):
            blk = lg_ref.at[q, y_peer]
            arrived(blk, rx.at[1])
            remote(blk, blk, tx.at[2], rx.at[3], row, core_peer).start()

        def share_end(q, rx):
            arrived(lg_ref.at[q, core_peer], rx.at[2])
            arrived(lg_ref.at[q, far], rx.at[3])

        def b0_arrived(c):
            arrived(rb_ref.at[0, c], b0_rx.at[c])

        for k, c in mid_order(lead):
            blk = rb_ref.at[k, c]
            if k == 1:
                remote(own_chunk(c), blk, b_tx, b1_rx.at[c], 2, col).start()
                continue
            b0_arrived(c)
            remote(blk, blk, fwd_tx, b0_rx.at[c], 2, col).start()
            if c == chunks // 2:
                l_forward()
                arrived(lg_ref.at[2, col], l2_rx.at[0])
                share(2, l2_rx, l2_tx)
        for c in range(lead, chunks):
            b0_arrived(c)
        arrived(lg_ref.at[1, col], l3_rx.at[0])
        share(1, l3_rx, l3_tx)
        share_forward(2, l2_rx, l2_tx)
        share_end(2, l2_rx)

        def last_loads(blocks):
            return [load(lead + j, j, k, ref(lead + j)) for j in range(LAST) for k, ref in blocks]

        b012 = [(0, lambda c: rb_ref.at[0, c]), (1, own_chunk), (2, lambda c: rb_ref.at[1, c])]
        b3 = [(3, lambda c: rb_ref.at[2, c])]

        def send_last(q, r):
            def one(t, carry):
                i, j = lax.rem(t, TILES), t // TILES
                remote(xs_v.at[q, j, i], x_tile(i, lead + j), xs_tx.at[q], xs_rx.at[q], r, col).start()
                return carry

            lax.fori_loop(0, TILES * LAST if q == 0 else TILES * (LAST - 1), one, 0)

        for c in range(lead, chunks):
            arrived(rb_ref.at[1, c], b1_rx.at[c])
        for cp in last_loads(b012):
            cp.start()

        def last_strip(i):
            part = lax.rem(i, 2)
            return [
                pltpu.make_async_copy(
                    lg_ref.at[2, k, tile_rows(i)], strip_v.at[part, :, pl.ds(k * n, n)], strip_sem.at[part]
                )
                for k in range(3)
            ]

        for cp in last_strip(0):
            cp.start()
        for cp in last_loads(b012):
            cp.wait()

        def tile2(i, carry):
            for cp in last_strip(i):
                cp.wait()

            @pl.when(i + 1 < TILES)
            def _():
                for cp in last_strip(i + 1):
                    cp.start()

            for j in range(LAST):
                xs_v[0, j, i] = dot(strip_v[lax.rem(i, 2)], b_v[j, : 3 * n, :]).astype(xs_v.dtype)
            return carry

        lax.fori_loop(0, TILES, tile2, 0)
        send_last(0, 2)

        l_exchange_end()
        simple_rows(1, [(0, lambda c: rb_ref.at[0, c]), (1, own_chunk)])

        share_forward(1, l3_rx, l3_tx)
        share_end(1, l3_rx)
        l3_load()
        for c in range(lead, chunks):
            arrived(rb_ref.at[2, c], b3_rx.at[c])
        for cp in last_loads(b012 + b3):
            cp.start()
        for cp in last_loads(b012 + b3):
            cp.wait()
        arrived(l3_v, l3_sem)

        def tile3(i, carry):
            for j in range(LAST):
                xs_v[1, j, i] = dot(l3_v[tile_rows(i), :], b_v[j]).astype(xs_v.dtype)
            return carry

        lax.fori_loop(0, TILES, tile3, 0)
        send_last(1, 3)
        for i in range(TILES):
            pltpu.make_async_copy(xs_v.at[1, LAST - 1, i], t_ref.at[pl.ds(i * rt, rt)], xs_tx.at[2]).start()

        l_exchange_drain()
        for s in range(3):
            arrived(l_ref, l2_tx.at[s])
            arrived(l_ref, l3_tx.at[s])
        arrived(lead_part(b_ref), b_tx)
        arrived(lead_part(b_ref), fwd_tx)
        arrived(xs_v.at[0], xs_tx.at[0])
        arrived(xs_v.at[1, pl.ds(0, LAST - 1)], xs_tx.at[1])
        arrived(t_ref, xs_tx.at[2])

    @pl.when(row == 2)
    def _():
        l_exchange_start()
        lo, hi = pl.ds(0, half), pl.ds(half, half)

        def own(p):
            return lg_ref.at[1, col, p]

        def other(p):
            return lg_ref.at[1, y_peer, p]

        remote(l_ref, lg_ref.at[2, col], l2_tx.at[0], l2_rx.at[0], 1, col).start()
        for c in range(lead, chunks):
            remote(own_chunk(c), rb_ref.at[1, c], b_tx, b1_rx.at[c], 1, col).start()

        arrived(own(lo), l3_rx.at[0])
        remote(own(lo), own(lo), l3_tx.at[0], l3_rx.at[2], row, y_peer).start()
        remote(own(lo), own(lo), l3_tx.at[1], l3_rx.at[4], row, core_peer).start()
        arrived(own(hi), l3_rx.at[1])
        remote(lg_ref.at[1, col], lg_ref.at[1, col], l2_tx.at[1], l3_rx.at[0], 1, col).start()
        remote(own(hi), own(hi), l3_tx.at[2], l3_rx.at[5], row, core_peer).start()
        l_forward()
        arrived(other(lo), l3_rx.at[2])
        remote(other(lo), other(lo), l3_tx.at[3], l3_rx.at[6], row, core_peer).start()
        arrived(other(hi), l3_rx.at[3])
        remote(other(hi), other(hi), l3_tx.at[4], l3_rx.at[7], row, core_peer).start()
        l_exchange_end()
        for s, (blk, p) in enumerate(((core_peer, lo), (core_peer, hi), (far, lo), (far, hi))):
            arrived(lg_ref.at[1, blk, p], l3_rx.at[4 + s])
        l3_load()

        def early(c, slot):
            return (
                load(c, slot, 1, rb_ref.at[1, c]), load(c, slot, 2, own_chunk(c)), load(c, slot, 3, rb_ref.at[2, c])
            )

        def prefetch(c, slot):
            arrived(rb_ref.at[1, c], b1_rx.at[c])
            arrived(rb_ref.at[2, c], b3_rx.at[c])
            for cp in early(c, slot):
                cp.start()

        def x3_send(i, c, slot):
            return remote(x3_v.at[slot, i], x_tile(i, c), x3_tx.at[slot, i], x3_rx, 3, col)

        prefetch(0, 0)
        strip_start(2, 0)
        pltpu.make_async_copy(l3_v, l3_v, l3_sem).wait()

        def step(c, carry):
            slot = lax.rem(c, 2)
            arrived(rb_ref.at[0, c], b0_rx.at[c])
            last = load(c, slot, 0, rb_ref.at[0, c])
            last.start()
            for cp in (*early(c, slot), last):
                cp.wait()
            def tile(i, inner):
                @pl.when(c >= 2)
                def _():
                    x3_send(i, c, slot).wait_send()

                rows = pl.ds(pl.multiple_of(i * rt, rt), rt)
                x3_v[slot, i] = jnp.dot(
                    l3_v[rows, :], b_v[slot], preferred_element_type=jnp.float32
                ).astype(x3_v.dtype)

                @pl.when(i > 0)
                def _():
                    x3_send(i - 1, c, slot).start()

                return inner

            lax.fori_loop(0, TILES, tile, 0)

            x3_send(TILES - 1, c, slot).start()

            @pl.when(c + 1 < lead)
            def _():
                prefetch(c + 1, 1 - slot)

            own_rows(2, c, slot, lead)
            return carry

        lax.fori_loop(0, lead, step, 0)
        own_rows_drain()
        for s in range(2):
            for i in range(TILES):
                x3_send(i, 0, s).wait_send()
        arrived(last_part(x_ref), xs_rx.at[0])
        for s in range(2):
            arrived(l_ref, l2_tx.at[s])
        arrived(last_part(b_ref), b_tx)
        l_exchange_drain()
        for s in range(5):
            arrived(own(lo), l3_tx.at[s])

    @pl.when(row == 3)
    def _():
        lo, hi = pl.ds(0, half), pl.ds(half, half)
        for s, p in enumerate((lo, hi)):
            remote(l_ref.at[p], lg_ref.at[1, col, p], l3_tx.at[s], l3_rx.at[s], 2, col).start()
        remote(l_ref.at[hi], lg_ref.at[1, col, hi], l3_tx.at[2], cross_rx, row, y_peer).start()
        blk = lg_ref.at[1, y_peer, hi]
        arrived(blk, cross_rx)
        remote(blk, blk, l3_tx.at[3], l3_rx.at[3], 2, col).start()

        def send(first, end, r):
            def one(c, carry):
                remote(own_chunk(c), rb_ref.at[2, c], b_tx, b3_rx.at[c], r, col).start()
                return carry

            lax.fori_loop(first, end, one, 0)

        mark = lead * 5 // 7
        send(0, mark, 2)
        send(lead, chunks, 1)
        send(mark, lead, 2)
        for s in range(4):
            arrived(blk, l3_tx.at[s])
        arrived(b_ref, b_tx)
        arrived(lead_part(x_ref), x3_rx)
        arrived(x_ref.at[:, pl.ds(lead * w, LAST * w - TAIL)], xs_rx.at[1])


def copy_kernel(src_ref, dst_ref, buf, in_sem, out_sem):
    parts, rows, _ = buf.shape

    def fetch(s):
        return pltpu.make_async_copy(src_ref.at[pl.ds(s * rows, rows)], buf.at[s], in_sem.at[s])

    def store(s):
        return pltpu.make_async_copy(buf.at[s], dst_ref.at[pl.ds(s * rows, rows)], out_sem.at[s])

    for s in range(parts):
        fetch(s).start()
    for s in range(parts):
        fetch(s).wait()
        store(s).start()
    for s in range(parts):
        store(s).wait()


def tail_kernel(x_ref, tail_ref, out_ref, sem):
    del x_ref

    @pl.when(lax.axis_index("row") == 3)
    def _():
        store = pltpu.make_async_copy(tail_ref, out_ref.at[:, pl.ds(out_ref.shape[1] - TAIL, TAIL)], sem)
        store.start()
        store.wait()


def solution(mesh):
    block_spec = P(("batch", "row"), "col")

    def local_product(l_block, b_block):
        n, m = b_block.shape
        rt = n // TILES
        chunks = m // CHUNK
        dma = pltpu.SemaphoreType.DMA
        hbm = pl.BlockSpec(memory_space=pl.ANY)
        x, _, _, tail = pl.pallas_call(
            kernel,
            out_shape=(
                jax.ShapeDtypeStruct((n, m), b_block.dtype),
                jax.ShapeDtypeStruct((3, chunks, n, CHUNK), b_block.dtype),
                jax.ShapeDtypeStruct((3, 4, n, n), l_block.dtype),
                jax.ShapeDtypeStruct((n, TAIL), b_block.dtype),
            ),
            in_specs=[hbm, hbm],
            out_specs=(hbm, hbm, hbm, hbm),
            scratch_shapes=[
                pltpu.VMEM((n, 4 * n), l_block.dtype),
                pltpu.VMEM((2, 4 * n, CHUNK), b_block.dtype),
                pltpu.VMEM((2, rt, 3 * n), l_block.dtype),
                pltpu.VMEM((2, TILES, rt, CHUNK), b_block.dtype),
                pltpu.VMEM((2, rt, CHUNK), b_block.dtype),
                pltpu.VMEM((2, LAST, TILES, rt, CHUNK), b_block.dtype),
                dma((chunks,)), dma((chunks,)), dma((chunks,)), dma((3,)), dma((4,)), dma((8,)), dma, dma, dma((2,)),
                dma, dma, dma((3,)), dma((3,)), dma((5,)), dma((2, TILES)), dma((3,)),
                dma((2, 4)), dma((2,)), dma((2,)), dma,
            ],
            compiler_params=pltpu.CompilerParams(has_side_effects=True, collective_id=0, vmem_limit_bytes=66 * 1000 * 1000),
        )(l_block, b_block)
        tail = lax.ppermute(tail, "row", [(1, 3)])
        x = pl.pallas_call(
            copy_kernel,
            out_shape=jax.ShapeDtypeStruct((n, m), x.dtype),
            in_specs=[hbm],
            out_specs=hbm,
            scratch_shapes=[pltpu.VMEM((PARTS, n // PARTS, m), x.dtype), dma((PARTS,)), dma((PARTS,))],
            compiler_params=pltpu.CompilerParams(vmem_limit_bytes=66 * 1000 * 1000),
            cost_estimate=pl.CostEstimate(flops=4 * 10**9, bytes_accessed=4 * n * m, transcendentals=0),
        )(x)
        return pl.pallas_call(
            tail_kernel,
            out_shape=jax.ShapeDtypeStruct((n, m), x.dtype),
            in_specs=[hbm, pl.BlockSpec(memory_space=pltpu.VMEM)],
            out_specs=hbm,
            input_output_aliases={0: 0},
            scratch_shapes=[dma],
        )(x, tail)

    return jax.shard_map(
        local_product, mesh=mesh, in_specs=(block_spec, block_spec), out_specs=block_spec, check_vma=False
    )
```

```python
import functools

import jax
import jax.numpy as jnp
from jax import lax
from jax.experimental import pallas as pl
from jax.experimental.pallas import tpu as pltpu
from jax.sharding import PartitionSpec as P

MESH = pl.DeviceIdType.MESH
PARTS = 8
TILES = 4
CHUNK = 256
TAIL = 256
LAST = 2


def mid_order(lead):
    first = lead - 2
    late = list(range(first, lead))
    gap = -(-lead // 3)
    order = [(1, c) for c in range(first)]
    for c in range(lead):
        order.append((0, c))
        if late and (c + 1) % gap == 0:
            order.append((1, late.pop(0)))
    assert not late
    return order


def kernel(
    l_ref, b_ref, x_ref, rb_ref, lg_ref, t_ref,
    l3_v, b_v, strip_v, x3_v, xo_v, xs_v,
    b0_rx, b1_rx, b3_rx, l_rx, l2_rx, l3_rx, cross_rx, x3_rx, xs_rx,
    b_tx, fwd_tx, l_tx, l2_tx, l3_tx, x3_tx, xs_tx,
    load_sem, strip_sem, out_sem, l3_sem,
):
    n, m = b_ref.shape
    half = n // 2
    rt = n // TILES
    w = CHUNK
    chunks = m // w
    lead = chunks - LAST
    batch, row, col = (lax.axis_index(a) for a in ("batch", "row", "col"))
    core_peer = col + 1 - 2 * lax.rem(col, 2)
    y_peer = lax.rem(col + 2, 4)
    far = lax.rem(core_peer + 2, 4)

    def remote(src, dst, send, recv, r, c):
        return pltpu.make_async_remote_copy(
            src_ref=src, dst_ref=dst, send_sem=send, recv_sem=recv,
            device_id=(batch, r, c), device_id_type=MESH,
        )

    def arrived(dst, sem):
        pltpu.make_async_copy(dst, dst, sem).wait()

    def lead_part(ref):
        return ref.at[:, pl.ds(0, lead * w)]

    def last_part(ref):
        return ref.at[:, pl.ds(lead * w, LAST * w)]

    def dot(a, b):
        return jnp.dot(a, b, preferred_element_type=jnp.float32)

    def tile_rows(i):
        return pl.ds(pl.multiple_of(i * rt, rt), rt)

    def l3_load():
        for k in range(4):
            pltpu.make_async_copy(lg_ref.at[1, k], l3_v.at[:, pl.ds(k * n, n)], l3_sem).start()

    def own_chunk(c):
        return b_ref.at[:, pl.ds(pl.multiple_of(c * w, w), w)]

    def x_tile(i, c):
        return x_ref.at[pl.ds(pl.multiple_of(i * rt, rt), rt), pl.ds(pl.multiple_of(c * w, w), w)]

    barrier = pltpu.get_barrier_semaphore()
    greet = functools.partial(pl.semaphore_signal, barrier, inc=1, device_id_type=MESH)
    greet(device_id=(batch, row, core_peer))
    greet(device_id=(batch, row, y_peer))

    @pl.when(row > 0)
    def _():
        greet(device_id=(batch, row - 1, col))

    @pl.when(row < 3)
    def _():
        greet(device_id=(batch, row + 1, col))

    @pl.when((row == 1) | (row == 3))
    def _():
        greet(device_id=(batch, 4 - row, col))

    pl.semaphore_wait(barrier, 3 + jnp.where(row == 0, 0, jnp.where(row == 1, 2, 1)))

    def l_exchange_start():
        remote(l_ref, lg_ref.at[0, col], l_tx.at[0], l_rx.at[0], row, y_peer).start()
        remote(l_ref, lg_ref.at[0, col], l_tx.at[1], l_rx.at[1], row, core_peer).start()

    def l_forward():
        blk = lg_ref.at[0, y_peer]
        arrived(blk, l_rx.at[0])
        remote(blk, blk, l_tx.at[2], l_rx.at[2], row, core_peer).start()

    def l_exchange_end():
        arrived(lg_ref.at[0, core_peer], l_rx.at[1])
        arrived(lg_ref.at[0, far], l_rx.at[2])

    def l_exchange_drain():
        for s in range(3):
            arrived(l_ref, l_tx.at[s])

    def strip_start(r, i):
        slot = lax.rem(i, 2)
        rows = pl.ds(pl.multiple_of(i * rt, rt), rt)
        for k in range(r + 1):
            dst = strip_v.at[slot, :, pl.ds(k * n, n)]

            @pl.when(col == k)
            def _(dst=dst):
                pltpu.make_async_copy(l_ref.at[rows], dst, strip_sem.at[slot]).start()

            @pl.when(col != k)
            def _(dst=dst, k=k):
                pltpu.make_async_copy(lg_ref.at[0, k, rows], dst, strip_sem.at[slot]).start()

    def strip_wait(r, i):
        slot = lax.rem(i, 2)
        ref = strip_v.at[slot, :, pl.ds(0, (r + 1) * n)]
        pltpu.make_async_copy(ref, ref, strip_sem.at[slot]).wait()

    def load(c, slot, k, src):
        return pltpu.make_async_copy(src, b_v.at[slot, pl.ds(k * n, n), :], load_sem.at[slot, k])

    def own_rows(r, c, slot, end):
        depth = (r + 1) * n

        def tile(i, carry):
            part = lax.rem(i, 2)
            strip_wait(r, i)

            @pl.when((i + 1 < TILES) | (c + 1 < end))
            def _():
                strip_start(r, lax.rem(i + 1, TILES))

            out = pltpu.make_async_copy(xo_v.at[part], x_tile(i, c), out_sem.at[part])

            @pl.when((i >= 2) | (c > 0))
            def _():
                out.wait()

            xo_v[part] = jnp.dot(
                strip_v[part, :, :depth], b_v[slot, :depth, :], preferred_element_type=jnp.float32
            ).astype(xo_v.dtype)
            out.start()
            return carry

        lax.fori_loop(0, TILES, tile, 0)

    def own_rows_drain():
        for s in range(2):
            pltpu.make_async_copy(xo_v.at[s], x_tile(s, 0), out_sem.at[s]).wait()

    def simple_rows(r, prior):
        def loads(c, slot):
            return [load(c, slot, k, ref(c)) for k, ref in prior]

        for cp in loads(0, 0):
            cp.start()
        strip_start(r, 0)

        def step(c, carry):
            slot = lax.rem(c, 2)
            for cp in loads(c, slot):
                cp.wait()

            @pl.when(c + 1 < chunks)
            def _():
                for cp in loads(c + 1, 1 - slot):
                    cp.start()

            own_rows(r, c, slot, chunks)
            return carry

        lax.fori_loop(0, chunks, step, 0)
        own_rows_drain()

    @pl.when(row == 0)
    def _():
        def send(c, carry):
            remote(own_chunk(c), rb_ref.at[0, c], b_tx, b0_rx.at[c], 1, col).start()
            return carry

        lax.fori_loop(0, chunks, send, 0)
        l_exchange_start()
        l_forward()
        l_exchange_end()
        simple_rows(0, [(0, own_chunk)])
        l_exchange_drain()
        arrived(b_ref, b_tx)

    @pl.when(row == 1)
    def _():
        l_exchange_start()

        def share(q, rx, tx):
            own = lg_ref.at[q, col]
            remote(own, own, tx.at[0], rx.at[1], row, y_peer).start()
            remote(own, own, tx.at[1], rx.at[2], row, core_peer).start()

        def share_forward(q, rx, tx):
            blk = lg_ref.at[q, y_peer]
            arrived(blk, rx.at[1])
            remote(blk, blk, tx.at[2], rx.at[3], row, core_peer).start()

        def share_end(q, rx):
            arrived(lg_ref.at[q, core_peer], rx.at[2])
            arrived(lg_ref.at[q, far], rx.at[3])

        def b0_arrived(c):
            arrived(rb_ref.at[0, c], b0_rx.at[c])

        for k, c in mid_order(lead):
            blk = rb_ref.at[k, c]
            if k == 1:
                remote(own_chunk(c), blk, b_tx, b1_rx.at[c], 2, col).start()
                continue
            b0_arrived(c)
            remote(blk, blk, fwd_tx, b0_rx.at[c], 2, col).start()
            if c == chunks // 2:
                l_forward()
                arrived(lg_ref.at[2, col], l2_rx.at[0])
                share(2, l2_rx, l2_tx)
        for c in range(lead, chunks):
            b0_arrived(c)
        arrived(lg_ref.at[1, col], l3_rx.at[0])
        share(1, l3_rx, l3_tx)
        share_forward(2, l2_rx, l2_tx)
        share_end(2, l2_rx)

        def last_loads(blocks):
            return [load(lead + j, j, k, ref(lead + j)) for j in range(LAST) for k, ref in blocks]

        b012 = [(0, lambda c: rb_ref.at[0, c]), (1, own_chunk), (2, lambda c: rb_ref.at[1, c])]
        b3 = [(3, lambda c: rb_ref.at[2, c])]

        def send_last(q, r, j):
            def one(i, carry):
                remote(xs_v.at[q, j, i], x_tile(i, lead + j), xs_tx.at[q], xs_rx.at[q], r, col).start()
                return carry

            lax.fori_loop(0, TILES, one, 0)

        for c in range(lead, chunks):
            arrived(rb_ref.at[1, c], b1_rx.at[c])
        for cp in last_loads(b012):
            cp.start()

        def last_strip(i):
            part = lax.rem(i, 2)
            return [
                pltpu.make_async_copy(
                    lg_ref.at[2, k, tile_rows(i)], strip_v.at[part, :, pl.ds(k * n, n)], strip_sem.at[part]
                )
                for k in range(3)
            ]

        for cp in last_strip(0):
            cp.start()
        for cp in last_loads(b012):
            cp.wait()

        def tile2(i, carry):
            for cp in last_strip(i):
                cp.wait()

            @pl.when(i + 1 < TILES)
            def _():
                for cp in last_strip(i + 1):
                    cp.start()

            for j in range(LAST):
                xs_v[0, j, i] = dot(strip_v[lax.rem(i, 2)], b_v[j, : 3 * n, :]).astype(xs_v.dtype)
            return carry

        lax.fori_loop(0, TILES, tile2, 0)
        send_last(0, 2, 0)

        l_exchange_end()
        simple_rows(1, [(0, lambda c: rb_ref.at[0, c]), (1, own_chunk)])

        share_forward(1, l3_rx, l3_tx)
        share_end(1, l3_rx)
        l3_load()
        for c in range(lead, chunks):
            arrived(rb_ref.at[2, c], b3_rx.at[c])
        for cp in last_loads(b012 + b3):
            cp.start()
        for cp in last_loads(b012 + b3):
            cp.wait()
        arrived(l3_v, l3_sem)

        def tile3(i, carry):
            for j in range(LAST):
                xs_v[1, j, i] = dot(l3_v[tile_rows(i), :], b_v[j]).astype(xs_v.dtype)
            return carry

        lax.fori_loop(0, TILES, tile3, 0)
        for j in range(LAST - 1):
            send_last(1, 3, j)
        for j in range(1, LAST):
            send_last(0, 2, j)
        for i in range(TILES):
            pltpu.make_async_copy(xs_v.at[1, LAST - 1, i], t_ref.at[pl.ds(i * rt, rt)], xs_tx.at[2]).start()

        l_exchange_drain()
        for s in range(3):
            arrived(l_ref, l2_tx.at[s])
            arrived(l_ref, l3_tx.at[s])
        arrived(lead_part(b_ref), b_tx)
        arrived(lead_part(b_ref), fwd_tx)
        arrived(xs_v.at[0], xs_tx.at[0])
        arrived(xs_v.at[1, pl.ds(0, LAST - 1)], xs_tx.at[1])
        arrived(t_ref, xs_tx.at[2])

    @pl.when(row == 2)
    def _():
        l_exchange_start()
        lo, hi = pl.ds(0, half), pl.ds(half, half)

        def own(p):
            return lg_ref.at[1, col, p]

        def other(p):
            return lg_ref.at[1, y_peer, p]

        remote(l_ref, lg_ref.at[2, col], l2_tx.at[0], l2_rx.at[0], 1, col).start()
        for c in range(lead, chunks):
            remote(own_chunk(c), rb_ref.at[1, c], b_tx, b1_rx.at[c], 1, col).start()

        arrived(own(lo), l3_rx.at[0])
        remote(own(lo), own(lo), l3_tx.at[0], l3_rx.at[2], row, y_peer).start()
        remote(own(lo), own(lo), l3_tx.at[1], l3_rx.at[4], row, core_peer).start()
        arrived(own(hi), l3_rx.at[1])
        remote(lg_ref.at[1, col], lg_ref.at[1, col], l2_tx.at[1], l3_rx.at[0], 1, col).start()
        remote(own(hi), own(hi), l3_tx.at[2], l3_rx.at[5], row, core_peer).start()
        l_forward()
        arrived(other(lo), l3_rx.at[2])
        remote(other(lo), other(lo), l3_tx.at[3], l3_rx.at[6], row, core_peer).start()
        arrived(other(hi), l3_rx.at[3])
        remote(other(hi), other(hi), l3_tx.at[4], l3_rx.at[7], row, core_peer).start()
        l_exchange_end()
        for s, (blk, p) in enumerate(((core_peer, lo), (core_peer, hi), (far, lo), (far, hi))):
            arrived(lg_ref.at[1, blk, p], l3_rx.at[4 + s])
        l3_load()

        def early(c, slot):
            return (
                load(c, slot, 1, rb_ref.at[1, c]), load(c, slot, 2, own_chunk(c)), load(c, slot, 3, rb_ref.at[2, c])
            )

        def prefetch(c, slot):
            arrived(rb_ref.at[1, c], b1_rx.at[c])
            arrived(rb_ref.at[2, c], b3_rx.at[c])
            for cp in early(c, slot):
                cp.start()

        def x3_send(i, c, slot):
            return remote(x3_v.at[slot, i], x_tile(i, c), x3_tx.at[slot, i], x3_rx, 3, col)

        prefetch(0, 0)
        strip_start(2, 0)
        pltpu.make_async_copy(l3_v, l3_v, l3_sem).wait()

        def step(c, carry):
            slot = lax.rem(c, 2)
            arrived(rb_ref.at[0, c], b0_rx.at[c])
            last = load(c, slot, 0, rb_ref.at[0, c])
            last.start()
            for cp in (*early(c, slot), last):
                cp.wait()
            def tile(i, inner):
                @pl.when(c >= 2)
                def _():
                    x3_send(i, c, slot).wait_send()

                rows = pl.ds(pl.multiple_of(i * rt, rt), rt)
                x3_v[slot, i] = jnp.dot(
                    l3_v[rows, :], b_v[slot], preferred_element_type=jnp.float32
                ).astype(x3_v.dtype)

                @pl.when(i > 0)
                def _():
                    x3_send(i - 1, c, slot).start()

                return inner

            lax.fori_loop(0, TILES, tile, 0)

            x3_send(TILES - 1, c, slot).start()

            @pl.when(c + 1 < lead)
            def _():
                prefetch(c + 1, 1 - slot)

            own_rows(2, c, slot, lead)
            return carry

        lax.fori_loop(0, lead, step, 0)
        own_rows_drain()
        for s in range(2):
            for i in range(TILES):
                x3_send(i, 0, s).wait_send()
        arrived(last_part(x_ref), xs_rx.at[0])
        for s in range(2):
            arrived(l_ref, l2_tx.at[s])
        arrived(last_part(b_ref), b_tx)
        l_exchange_drain()
        for s in range(5):
            arrived(own(lo), l3_tx.at[s])

    @pl.when(row == 3)
    def _():
        lo, hi = pl.ds(0, half), pl.ds(half, half)
        for s, p in enumerate((lo, hi)):
            remote(l_ref.at[p], lg_ref.at[1, col, p], l3_tx.at[s], l3_rx.at[s], 2, col).start()
        remote(l_ref.at[hi], lg_ref.at[1, col, hi], l3_tx.at[2], cross_rx, row, y_peer).start()
        blk = lg_ref.at[1, y_peer, hi]
        arrived(blk, cross_rx)
        remote(blk, blk, l3_tx.at[3], l3_rx.at[3], 2, col).start()

        def send(first, end, r):
            def one(c, carry):
                remote(own_chunk(c), rb_ref.at[2, c], b_tx, b3_rx.at[c], r, col).start()
                return carry

            lax.fori_loop(first, end, one, 0)

        mark = lead * 5 // 7
        send(0, mark, 2)
        send(lead, chunks, 1)
        send(mark, lead, 2)
        for s in range(4):
            arrived(blk, l3_tx.at[s])
        arrived(b_ref, b_tx)
        arrived(lead_part(x_ref), x3_rx)
        arrived(x_ref.at[:, pl.ds(lead * w, LAST * w - TAIL)], xs_rx.at[1])


def copy_kernel(src_ref, dst_ref, buf, in_sem, out_sem):
    parts, rows, _ = buf.shape

    def fetch(s):
        return pltpu.make_async_copy(src_ref.at[pl.ds(s * rows, rows)], buf.at[s], in_sem.at[s])

    def store(s):
        return pltpu.make_async_copy(buf.at[s], dst_ref.at[pl.ds(s * rows, rows)], out_sem.at[s])

    for s in range(parts):
        fetch(s).start()
    for s in range(parts):
        fetch(s).wait()
        store(s).start()
    for s in range(parts):
        store(s).wait()


def tail_kernel(x_ref, tail_ref, out_ref, sem):
    del x_ref

    @pl.when(lax.axis_index("row") == 3)
    def _():
        store = pltpu.make_async_copy(tail_ref, out_ref.at[:, pl.ds(out_ref.shape[1] - TAIL, TAIL)], sem)
        store.start()
        store.wait()


def solution(mesh):
    block_spec = P(("batch", "row"), "col")

    def local_product(l_block, b_block):
        n, m = b_block.shape
        rt = n // TILES
        chunks = m // CHUNK
        dma = pltpu.SemaphoreType.DMA
        hbm = pl.BlockSpec(memory_space=pl.ANY)
        x, _, _, tail = pl.pallas_call(
            kernel,
            out_shape=(
                jax.ShapeDtypeStruct((n, m), b_block.dtype),
                jax.ShapeDtypeStruct((3, chunks, n, CHUNK), b_block.dtype),
                jax.ShapeDtypeStruct((3, 4, n, n), l_block.dtype),
                jax.ShapeDtypeStruct((n, TAIL), b_block.dtype),
            ),
            in_specs=[hbm, hbm],
            out_specs=(hbm, hbm, hbm, hbm),
            scratch_shapes=[
                pltpu.VMEM((n, 4 * n), l_block.dtype),
                pltpu.VMEM((2, 4 * n, CHUNK), b_block.dtype),
                pltpu.VMEM((2, rt, 3 * n), l_block.dtype),
                pltpu.VMEM((2, TILES, rt, CHUNK), b_block.dtype),
                pltpu.VMEM((2, rt, CHUNK), b_block.dtype),
                pltpu.VMEM((2, LAST, TILES, rt, CHUNK), b_block.dtype),
                dma((chunks,)), dma((chunks,)), dma((chunks,)), dma((3,)), dma((4,)), dma((8,)), dma, dma, dma((2,)),
                dma, dma, dma((3,)), dma((3,)), dma((5,)), dma((2, TILES)), dma((3,)),
                dma((2, 4)), dma((2,)), dma((2,)), dma,
            ],
            compiler_params=pltpu.CompilerParams(has_side_effects=True, collective_id=0, vmem_limit_bytes=66 * 1000 * 1000),
        )(l_block, b_block)
        tail = lax.ppermute(tail, "row", [(1, 3)])
        x = pl.pallas_call(
            copy_kernel,
            out_shape=jax.ShapeDtypeStruct((n, m), x.dtype),
            in_specs=[hbm],
            out_specs=hbm,
            scratch_shapes=[pltpu.VMEM((PARTS, n // PARTS, m), x.dtype), dma((PARTS,)), dma((PARTS,))],
            compiler_params=pltpu.CompilerParams(vmem_limit_bytes=66 * 1000 * 1000),
            cost_estimate=pl.CostEstimate(flops=4 * 10**9, bytes_accessed=4 * n * m, transcendentals=0),
        )(x)
        return pl.pallas_call(
            tail_kernel,
            out_shape=jax.ShapeDtypeStruct((n, m), x.dtype),
            in_specs=[hbm, pl.BlockSpec(memory_space=pltpu.VMEM)],
            out_specs=hbm,
            input_output_aliases={0: 0},
            scratch_shapes=[dma],
        )(x, tail)

    return jax.shard_map(
        local_product, mesh=mesh, in_specs=(block_spec, block_spec), out_specs=block_spec, check_vma=False
    )
```

```python
import functools

import jax
import jax.numpy as jnp
from jax import lax
from jax.experimental import pallas as pl
from jax.experimental.pallas import tpu as pltpu
from jax.sharding import PartitionSpec as P

MESH = pl.DeviceIdType.MESH
PARTS = 8
TILES = 4
CHUNK = 256
TAIL = 256
LAST = 2


def mid_order(lead):
    first = lead - 2
    late = list(range(first, lead))
    gap = -(-lead // 3)
    order = [(1, c) for c in range(first)]
    for c in range(lead):
        order.append((0, c))
        if late and (c + 1) % gap == 0:
            order.append((1, late.pop(0)))
    assert not late
    return order


def kernel(
    l_ref, b_ref, x_ref, rb_ref, lg_ref, t_ref,
    l3_v, b_v, strip_v, x3_v, xo_v, xs_v,
    b0_rx, b1_rx, b3_rx, l_rx, l2_rx, l3_rx, cross_rx, x3_rx, xs_rx,
    b_tx, fwd_tx, l_tx, l2_tx, l3_tx, x3_tx, xs_tx,
    load_sem, strip_sem, out_sem, l3_sem,
):
    n, m = b_ref.shape
    half = n // 2
    rt = n // TILES
    w = CHUNK
    chunks = m // w
    lead = chunks - LAST
    batch, row, col = (lax.axis_index(a) for a in ("batch", "row", "col"))
    core_peer = col + 1 - 2 * lax.rem(col, 2)
    y_peer = lax.rem(col + 2, 4)
    far = lax.rem(core_peer + 2, 4)

    def remote(src, dst, send, recv, r, c):
        return pltpu.make_async_remote_copy(
            src_ref=src, dst_ref=dst, send_sem=send, recv_sem=recv,
            device_id=(batch, r, c), device_id_type=MESH,
        )

    def arrived(dst, sem):
        pltpu.make_async_copy(dst, dst, sem).wait()

    def lead_part(ref):
        return ref.at[:, pl.ds(0, lead * w)]

    def last_part(ref):
        return ref.at[:, pl.ds(lead * w, LAST * w)]

    def dot(a, b):
        return jnp.dot(a, b, preferred_element_type=jnp.float32)

    def tile_rows(i):
        return pl.ds(pl.multiple_of(i * rt, rt), rt)

    def l3_load():
        for k in range(4):
            pltpu.make_async_copy(lg_ref.at[1, k], l3_v.at[:, pl.ds(k * n, n)], l3_sem).start()

    def own_chunk(c):
        return b_ref.at[:, pl.ds(pl.multiple_of(c * w, w), w)]

    def x_tile(i, c):
        return x_ref.at[pl.ds(pl.multiple_of(i * rt, rt), rt), pl.ds(pl.multiple_of(c * w, w), w)]

    barrier = pltpu.get_barrier_semaphore()
    greet = functools.partial(pl.semaphore_signal, barrier, inc=1, device_id_type=MESH)
    greet(device_id=(batch, row, core_peer))
    greet(device_id=(batch, row, y_peer))

    @pl.when(row > 0)
    def _():
        greet(device_id=(batch, row - 1, col))

    @pl.when(row < 3)
    def _():
        greet(device_id=(batch, row + 1, col))

    @pl.when((row == 1) | (row == 3))
    def _():
        greet(device_id=(batch, 4 - row, col))

    pl.semaphore_wait(barrier, 3 + jnp.where(row == 0, 0, jnp.where(row == 1, 2, 1)))

    def l_exchange_start():
        remote(l_ref, lg_ref.at[0, col], l_tx.at[0], l_rx.at[0], row, y_peer).start()
        remote(l_ref, lg_ref.at[0, col], l_tx.at[1], l_rx.at[1], row, core_peer).start()

    def l_forward():
        blk = lg_ref.at[0, y_peer]
        arrived(blk, l_rx.at[0])
        remote(blk, blk, l_tx.at[2], l_rx.at[2], row, core_peer).start()

    def l_exchange_end():
        arrived(lg_ref.at[0, core_peer], l_rx.at[1])
        arrived(lg_ref.at[0, far], l_rx.at[2])

    def l_exchange_drain():
        for s in range(3):
            arrived(l_ref, l_tx.at[s])

    def strip_start(r, i):
        slot = lax.rem(i, 2)
        rows = pl.ds(pl.multiple_of(i * rt, rt), rt)
        for k in range(r + 1):
            dst = strip_v.at[slot, :, pl.ds(k * n, n)]

            @pl.when(col == k)
            def _(dst=dst):
                pltpu.make_async_copy(l_ref.at[rows], dst, strip_sem.at[slot]).start()

            @pl.when(col != k)
            def _(dst=dst, k=k):
                pltpu.make_async_copy(lg_ref.at[0, k, rows], dst, strip_sem.at[slot]).start()

    def strip_wait(r, i):
        slot = lax.rem(i, 2)
        ref = strip_v.at[slot, :, pl.ds(0, (r + 1) * n)]
        pltpu.make_async_copy(ref, ref, strip_sem.at[slot]).wait()

    def load(c, slot, k, src):
        return pltpu.make_async_copy(src, b_v.at[slot, pl.ds(k * n, n), :], load_sem.at[slot, k])

    def own_rows(r, c, slot, end):
        depth = (r + 1) * n

        def tile(i, carry):
            part = lax.rem(i, 2)
            strip_wait(r, i)

            @pl.when((i + 1 < TILES) | (c + 1 < end))
            def _():
                strip_start(r, lax.rem(i + 1, TILES))

            out = pltpu.make_async_copy(xo_v.at[part], x_tile(i, c), out_sem.at[part])

            @pl.when((i >= 2) | (c > 0))
            def _():
                out.wait()

            xo_v[part] = jnp.dot(
                strip_v[part, :, :depth], b_v[slot, :depth, :], preferred_element_type=jnp.float32
            ).astype(xo_v.dtype)
            out.start()
            return carry

        lax.fori_loop(0, TILES, tile, 0)

    def own_rows_drain():
        for s in range(2):
            pltpu.make_async_copy(xo_v.at[s], x_tile(s, 0), out_sem.at[s]).wait()

    def simple_rows(r, prior):
        def loads(c, slot):
            return [load(c, slot, k, ref(c)) for k, ref in prior]

        for cp in loads(0, 0):
            cp.start()
        strip_start(r, 0)

        def step(c, carry):
            slot = lax.rem(c, 2)
            for cp in loads(c, slot):
                cp.wait()

            @pl.when(c + 1 < chunks)
            def _():
                for cp in loads(c + 1, 1 - slot):
                    cp.start()

            own_rows(r, c, slot, chunks)
            return carry

        lax.fori_loop(0, chunks, step, 0)
        own_rows_drain()

    @pl.when(row == 0)
    def _():
        def send(c, carry):
            remote(own_chunk(c), rb_ref.at[0, c], b_tx, b0_rx.at[c], 1, col).start()
            return carry

        lax.fori_loop(0, chunks, send, 0)
        l_exchange_start()
        l_forward()
        l_exchange_end()
        simple_rows(0, [(0, own_chunk)])
        l_exchange_drain()
        arrived(b_ref, b_tx)

    @pl.when(row == 1)
    def _():
        l_exchange_start()

        def share(q, rx, tx):
            own = lg_ref.at[q, col]
            remote(own, own, tx.at[0], rx.at[1], row, y_peer).start()
            remote(own, own, tx.at[1], rx.at[2], row, core_peer).start()

        def share_forward(q, rx, tx):
            blk = lg_ref.at[q, y_peer]
            arrived(blk, rx.at[1])
            remote(blk, blk, tx.at[2], rx.at[3], row, core_peer).start()

        def share_end(q, rx):
            arrived(lg_ref.at[q, core_peer], rx.at[2])
            arrived(lg_ref.at[q, far], rx.at[3])

        def b0_arrived(c):
            arrived(rb_ref.at[0, c], b0_rx.at[c])

        for k, c in mid_order(lead):
            blk = rb_ref.at[k, c]
            if k == 1:
                remote(own_chunk(c), blk, b_tx, b1_rx.at[c], 2, col).start()
                continue
            b0_arrived(c)
            remote(blk, blk, fwd_tx, b0_rx.at[c], 2, col).start()
            if c == chunks // 2:
                l_forward()
                arrived(lg_ref.at[2, col], l2_rx.at[0])
                share(2, l2_rx, l2_tx)
        for c in range(lead, chunks):
            b0_arrived(c)
        arrived(lg_ref.at[1, col], l3_rx.at[0])
        share(1, l3_rx, l3_tx)
        share_forward(2, l2_rx, l2_tx)
        share_end(2, l2_rx)

        def last_loads(blocks):
            return [load(lead + j, j, k, ref(lead + j)) for j in range(LAST) for k, ref in blocks]

        b012 = [(0, lambda c: rb_ref.at[0, c]), (1, own_chunk), (2, lambda c: rb_ref.at[1, c])]
        b3 = [(3, lambda c: rb_ref.at[2, c])]

        def send_last(q, r, j):
            def one(i, carry):
                remote(xs_v.at[q, j, i], x_tile(i, lead + j), xs_tx.at[q], xs_rx.at[q], r, col).start()
                return carry

            lax.fori_loop(0, TILES, one, 0)

        for c in range(lead, chunks):
            arrived(rb_ref.at[1, c], b1_rx.at[c])
        for cp in last_loads(b012):
            cp.start()

        def last_strip(i):
            part = lax.rem(i, 2)
            return [
                pltpu.make_async_copy(
                    lg_ref.at[2, k, tile_rows(i)], strip_v.at[part, :, pl.ds(k * n, n)], strip_sem.at[part]
                )
                for k in range(3)
            ]

        for cp in last_strip(0):
            cp.start()
        for cp in last_loads(b012):
            cp.wait()

        def tile2(i, carry):
            for cp in last_strip(i):
                cp.wait()

            @pl.when(i + 1 < TILES)
            def _():
                for cp in last_strip(i + 1):
                    cp.start()

            for j in range(LAST):
                xs_v[0, j, i] = dot(strip_v[lax.rem(i, 2)], b_v[j, : 3 * n, :]).astype(xs_v.dtype)
            return carry

        lax.fori_loop(0, TILES, tile2, 0)
        send_last(0, 2, 0)

        l_exchange_end()
        simple_rows(1, [(0, lambda c: rb_ref.at[0, c]), (1, own_chunk)])

        share_forward(1, l3_rx, l3_tx)
        share_end(1, l3_rx)
        l3_load()
        for c in range(lead, chunks):
            arrived(rb_ref.at[2, c], b3_rx.at[c])
        for cp in last_loads(b012 + b3):
            cp.start()
        for cp in last_loads(b012 + b3):
            cp.wait()
        arrived(l3_v, l3_sem)

        def tile3(i, carry):
            for j in range(LAST):
                xs_v[1, j, i] = dot(l3_v[tile_rows(i), :], b_v[j]).astype(xs_v.dtype)
            return carry

        lax.fori_loop(0, TILES, tile3, 0)
        for j in range(LAST):
            send_last(1, 3, j)
        for i in range(TILES):
            pltpu.make_async_copy(xs_v.at[0, LAST - 1, i], t_ref.at[pl.ds(i * rt, rt)], xs_tx.at[2]).start()

        l_exchange_drain()
        for s in range(3):
            arrived(l_ref, l2_tx.at[s])
            arrived(l_ref, l3_tx.at[s])
        arrived(lead_part(b_ref), b_tx)
        arrived(lead_part(b_ref), fwd_tx)
        arrived(xs_v.at[0, pl.ds(0, LAST - 1)], xs_tx.at[0])
        arrived(xs_v.at[1], xs_tx.at[1])
        arrived(t_ref, xs_tx.at[2])

    @pl.when(row == 2)
    def _():
        l_exchange_start()
        lo, hi = pl.ds(0, half), pl.ds(half, half)

        def own(p):
            return lg_ref.at[1, col, p]

        def other(p):
            return lg_ref.at[1, y_peer, p]

        remote(l_ref, lg_ref.at[2, col], l2_tx.at[0], l2_rx.at[0], 1, col).start()
        for c in range(lead, chunks):
            remote(own_chunk(c), rb_ref.at[1, c], b_tx, b1_rx.at[c], 1, col).start()

        arrived(own(lo), l3_rx.at[0])
        remote(own(lo), own(lo), l3_tx.at[0], l3_rx.at[2], row, y_peer).start()
        remote(own(lo), own(lo), l3_tx.at[1], l3_rx.at[4], row, core_peer).start()
        arrived(own(hi), l3_rx.at[1])
        remote(lg_ref.at[1, col], lg_ref.at[1, col], l2_tx.at[1], l3_rx.at[0], 1, col).start()
        remote(own(hi), own(hi), l3_tx.at[2], l3_rx.at[5], row, core_peer).start()
        l_forward()
        arrived(other(lo), l3_rx.at[2])
        remote(other(lo), other(lo), l3_tx.at[3], l3_rx.at[6], row, core_peer).start()
        arrived(other(hi), l3_rx.at[3])
        remote(other(hi), other(hi), l3_tx.at[4], l3_rx.at[7], row, core_peer).start()
        l_exchange_end()
        for s, (blk, p) in enumerate(((core_peer, lo), (core_peer, hi), (far, lo), (far, hi))):
            arrived(lg_ref.at[1, blk, p], l3_rx.at[4 + s])
        l3_load()

        def early(c, slot):
            return (
                load(c, slot, 1, rb_ref.at[1, c]), load(c, slot, 2, own_chunk(c)), load(c, slot, 3, rb_ref.at[2, c])
            )

        def prefetch(c, slot):
            arrived(rb_ref.at[1, c], b1_rx.at[c])
            arrived(rb_ref.at[2, c], b3_rx.at[c])
            for cp in early(c, slot):
                cp.start()

        def x3_send(i, c, slot):
            return remote(x3_v.at[slot, i], x_tile(i, c), x3_tx.at[slot, i], x3_rx, 3, col)

        prefetch(0, 0)
        strip_start(2, 0)
        pltpu.make_async_copy(l3_v, l3_v, l3_sem).wait()

        def step(c, carry):
            slot = lax.rem(c, 2)
            arrived(rb_ref.at[0, c], b0_rx.at[c])
            last = load(c, slot, 0, rb_ref.at[0, c])
            last.start()
            for cp in (*early(c, slot), last):
                cp.wait()
            def tile(i, inner):
                @pl.when(c >= 2)
                def _():
                    x3_send(i, c, slot).wait_send()

                rows = pl.ds(pl.multiple_of(i * rt, rt), rt)
                x3_v[slot, i] = jnp.dot(
                    l3_v[rows, :], b_v[slot], preferred_element_type=jnp.float32
                ).astype(x3_v.dtype)

                @pl.when(i > 0)
                def _():
                    x3_send(i - 1, c, slot).start()

                return inner

            lax.fori_loop(0, TILES, tile, 0)

            x3_send(TILES - 1, c, slot).start()

            @pl.when(c + 1 < lead)
            def _():
                prefetch(c + 1, 1 - slot)

            own_rows(2, c, slot, lead)
            return carry

        lax.fori_loop(0, lead, step, 0)
        own_rows_drain()
        for s in range(2):
            for i in range(TILES):
                x3_send(i, 0, s).wait_send()
        arrived(x_ref.at[:, pl.ds(lead * w, LAST * w - TAIL)], xs_rx.at[0])
        for s in range(2):
            arrived(l_ref, l2_tx.at[s])
        arrived(last_part(b_ref), b_tx)
        l_exchange_drain()
        for s in range(5):
            arrived(own(lo), l3_tx.at[s])

    @pl.when(row == 3)
    def _():
        lo, hi = pl.ds(0, half), pl.ds(half, half)
        for s, p in enumerate((lo, hi)):
            remote(l_ref.at[p], lg_ref.at[1, col, p], l3_tx.at[s], l3_rx.at[s], 2, col).start()
        remote(l_ref.at[hi], lg_ref.at[1, col, hi], l3_tx.at[2], cross_rx, row, y_peer).start()
        blk = lg_ref.at[1, y_peer, hi]
        arrived(blk, cross_rx)
        remote(blk, blk, l3_tx.at[3], l3_rx.at[3], 2, col).start()

        def send(first, end, r):
            def one(c, carry):
                remote(own_chunk(c), rb_ref.at[2, c], b_tx, b3_rx.at[c], r, col).start()
                return carry

            lax.fori_loop(first, end, one, 0)

        mark = lead * 5 // 7
        send(0, mark, 2)
        send(lead, chunks, 1)
        send(mark, lead, 2)
        for s in range(4):
            arrived(blk, l3_tx.at[s])
        arrived(b_ref, b_tx)
        arrived(lead_part(x_ref), x3_rx)
        arrived(last_part(x_ref), xs_rx.at[1])


def copy_kernel(src_ref, dst_ref, buf, in_sem, out_sem):
    parts, rows, _ = buf.shape

    def fetch(s):
        return pltpu.make_async_copy(src_ref.at[pl.ds(s * rows, rows)], buf.at[s], in_sem.at[s])

    def store(s):
        return pltpu.make_async_copy(buf.at[s], dst_ref.at[pl.ds(s * rows, rows)], out_sem.at[s])

    for s in range(parts):
        fetch(s).start()
    for s in range(parts):
        fetch(s).wait()
        store(s).start()
    for s in range(parts):
        store(s).wait()


def tail_kernel(x_ref, tail_ref, out_ref, sem):
    del x_ref

    @pl.when(lax.axis_index("row") == 2)
    def _():
        store = pltpu.make_async_copy(tail_ref, out_ref.at[:, pl.ds(out_ref.shape[1] - TAIL, TAIL)], sem)
        store.start()
        store.wait()


def solution(mesh):
    block_spec = P(("batch", "row"), "col")

    def local_product(l_block, b_block):
        n, m = b_block.shape
        rt = n // TILES
        chunks = m // CHUNK
        dma = pltpu.SemaphoreType.DMA
        hbm = pl.BlockSpec(memory_space=pl.ANY)
        x, _, _, tail = pl.pallas_call(
            kernel,
            out_shape=(
                jax.ShapeDtypeStruct((n, m), b_block.dtype),
                jax.ShapeDtypeStruct((3, chunks, n, CHUNK), b_block.dtype),
                jax.ShapeDtypeStruct((3, 4, n, n), l_block.dtype),
                jax.ShapeDtypeStruct((n, TAIL), b_block.dtype),
            ),
            in_specs=[hbm, hbm],
            out_specs=(hbm, hbm, hbm, hbm),
            scratch_shapes=[
                pltpu.VMEM((n, 4 * n), l_block.dtype),
                pltpu.VMEM((2, 4 * n, CHUNK), b_block.dtype),
                pltpu.VMEM((2, rt, 3 * n), l_block.dtype),
                pltpu.VMEM((2, TILES, rt, CHUNK), b_block.dtype),
                pltpu.VMEM((2, rt, CHUNK), b_block.dtype),
                pltpu.VMEM((2, LAST, TILES, rt, CHUNK), b_block.dtype),
                dma((chunks,)), dma((chunks,)), dma((chunks,)), dma((3,)), dma((4,)), dma((8,)), dma, dma, dma((2,)),
                dma, dma, dma((3,)), dma((3,)), dma((5,)), dma((2, TILES)), dma((3,)),
                dma((2, 4)), dma((2,)), dma((2,)), dma,
            ],
            compiler_params=pltpu.CompilerParams(has_side_effects=True, collective_id=0, vmem_limit_bytes=66 * 1000 * 1000),
        )(l_block, b_block)
        tail = lax.ppermute(tail, "row", [(1, 2)])
        x = pl.pallas_call(
            copy_kernel,
            out_shape=jax.ShapeDtypeStruct((n, m), x.dtype),
            in_specs=[hbm],
            out_specs=hbm,
            scratch_shapes=[pltpu.VMEM((PARTS, n // PARTS, m), x.dtype), dma((PARTS,)), dma((PARTS,))],
            compiler_params=pltpu.CompilerParams(vmem_limit_bytes=66 * 1000 * 1000),
            cost_estimate=pl.CostEstimate(flops=4 * 10**9, bytes_accessed=4 * n * m, transcendentals=0),
        )(x)
        return pl.pallas_call(
            tail_kernel,
            out_shape=jax.ShapeDtypeStruct((n, m), x.dtype),
            in_specs=[hbm, pl.BlockSpec(memory_space=pltpu.VMEM)],
            out_specs=hbm,
            input_output_aliases={0: 0},
            scratch_shapes=[dma],
        )(x, tail)

    return jax.shard_map(
        local_product, mesh=mesh, in_specs=(block_spec, block_spec), out_specs=block_spec, check_vma=False
    )
```
